32 devices in a mesh: dp: 16 (over z, x, core), tensor: 2 (over y).
Axes of the slice: x: 2, y: 2, z: 4, core: 2. Of those that a mesh axis runs over, the one named last changes fastest.
Arguments:
- grad_hidden: bfloat16 [2048, 14336], P('dp', 'tensor'), may hold values from -18 to 18
- gate: bfloat16 [2048, 14336], P('dp', 'tensor'), may hold values from -6 to 6
Outputs:
- factor: float32 [14336, 14336], P('tensor', 'dp')
The draws below stay inside these ranges and needn't reach their ends.
All inputs are finite; a program needn't handle non-finite values.
Results may differ from the reference program's by a relative error of at most 0.0065.
Values may be sent and summed in bfloat16 or wider, within the bound.
A program may use at most 128 MiB of HBM per device.

```python
import jax
import jax.numpy as jnp
from jax import lax

FF = 14336
TOKENS = 2048


def level_of(rng, extent, split, least, high):
    gain, own = 1.0, jax.random.fold_in(rng, 6)
    for dim, blocks in split:
        draws = jnp.exp(jax.random.uniform(jax.random.fold_in(own, dim), (blocks,), jnp.float32, least / len(split), high / len(split)))
        gain = gain * jnp.repeat(draws, extent[dim] // blocks).reshape([-1 if axis == dim else 1 for axis in range(len(extent))])
    return gain


def bell_draw(stream_key, dims, scale, most, shards=(), dtype=jnp.bfloat16):
    array = jax.random.normal(stream_key, dims, jnp.float32) * scale
    if len(shards) > 0:
        array = level_of(stream_key, dims, shards, -0.22, 0.18) * array
    return jnp.clip(array, min=-most, max=most).astype(dtype)


def setup_inputs(seed: int = 0) -> dict:
    splits = jax.random.split(jax.random.key(seed), 3)
    return {
        "grad_hidden": bell_draw(splits[0], (TOKENS, FF), 3.0, 18.0, ((0, 16), (1, 2))),
        "gate": bell_draw(splits[1], (TOKENS, FF), 1.0, 6.0, ((0, 16), (1, 2))),
    }


def reference(grad_hidden, gate):
    up_grad = (grad_hidden.astype(jnp.float32) * jax.nn.silu(gate.astype(jnp.float32))).astype(jnp.bfloat16)
    wide = up_grad.astype(jnp.float32)
    blocks = wide.reshape(wide.shape[0], FF // 1792 if FF % 1792 == 0 else 1, -1)
    blocks = jnp.transpose(blocks, (1, 0, 2))

    def column_block(piece):
        return jnp.dot(wide.T, piece, precision=lax.Precision.HIGHEST, preferred_element_type=jnp.float32)

    panels = lax.map(column_block, blocks)
    factor = jnp.transpose(panels, (1, 0, 2)).reshape(FF, FF)
    return factor / TOKENS
```

```python
import functools

import jax
import jax.numpy as jnp
from jax import lax
from jax.experimental import pallas as pl
from jax.experimental.pallas import tpu as pltpu
from jax.sharding import PartitionSpec as P

MESH = pl.DeviceIdType.MESH
LANES = 128
LINE = 4
CHIPS = 2 * LINE
VMEM_BYTES = 67_043_328

BOTTOM = {
    0: [(0, 0), (0, 1), (1, 0), (2, 0), (1, 1), (3, 0), (2, 1), (3, 1)],
    1: [(1, 0), (1, 1), (0, 0), (2, 0), (3, 0), (0, 1), (2, 1), (3, 1)],
}
ORDER = [BOTTOM[z] if z in BOTTOM else [(LINE - 1 - a, r) for a, r in BOTTOM[LINE - 1 - z]] for z in range(LINE)]
FIRST, SECOND = range(0, 5), range(5, 7)
LAST = CHIPS - 1


def activations(grad_hidden, gate):
    return (grad_hidden.astype(jnp.float32) * jax.nn.silu(gate.astype(jnp.float32))).astype(
        jnp.bfloat16
    )


def plain(grad_hidden, gate):
    up_grad = activations(grad_hidden, gate)
    tensor_count = lax.axis_size("tensor")
    data_count = lax.axis_size("dp")
    col_width = up_grad.shape[1] * tensor_count // data_count
    ratio = data_count // tensor_count
    data_index = lax.axis_index("dp")
    owner = data_index // ratio
    offset = data_index % ratio * col_width
    contract = (((0,), (0,)), ((), ()))
    total_tokens = up_grad.shape[0] * data_count
    rows_all = lax.all_gather(up_grad, "dp", axis=0, tiled=True)
    panel = lax.dynamic_slice_in_dim(rows_all, offset, col_width, 1)
    slices = lax.all_gather(panel, "tensor", axis=1, tiled=True)
    cols_all = lax.dynamic_slice_in_dim(slices, owner * col_width, col_width, 1)
    summed = lax.dot_general(rows_all, cols_all, contract, preferred_element_type=jnp.float32)
    return summed / total_tokens


def pick(index, values):
    known = [v for v in values if v is not None]
    if all(v == known[0] for v in known):
        return jnp.int32(known[0])
    out = jnp.int32(known[-1])
    for j, v in enumerate(values):
        if v is not None and v != known[-1]:
            out = jnp.where(index == j, v, out)
    return out


def slot_at(z, shift, d, r):
    def one(zz):
        if not (0 <= zz + d < LINE and 0 <= zz + shift < LINE):
            return None
        return ORDER[zz + shift].index((zz + d, r))
    return pick(z, [one(zz) for zz in range(LINE)])


def nt_dot(a, b):
    return lax.dot_general(a, b, (((1,), (1,)), ((), ())), preferred_element_type=jnp.float32)


def position():
    me, t = lax.axis_index("dp"), lax.axis_index("tensor")
    return me, t, me // 4, me // 2 % 2, me % 2


def gather_kernel(
    dims, g_ref, v_ref, all_ref, panel_ref, part_ref, g_buf, v_buf, g_sem, v_sem,
    z_send, x_send, c_send, y_send, recv, c_recv, y_recv,
):
    count, rows = dims
    me, t, z, x, core = position()
    here = me // 2
    half = CHIPS // 2
    owns = here // half == t
    part = here % half
    end = (z == 0) | (z == LINE - 1)
    has_up, has_down = z < LINE - 1, z > 0

    up = (jnp.minimum(z + 1, LINE - 1) * 4 + x * 2 + core, t)
    down = (jnp.maximum(z - 1, 0) * 4 + x * 2 + core, t)
    over = (z * 4 + (1 - x) * 2 + core, t)
    twin = (z * 4 + x * 2 + 1 - core, t)

    def chunk(i):
        return jnp.where(t == 0, i, count - 1 - i)

    def rows_of(k):
        return pl.ds(pl.multiple_of(k * rows, rows), rows)

    def inputs(i):
        columns = rows_of(chunk(i))
        return [
            pltpu.make_async_copy(src.at[:, columns], dst.at[:, columns], sem.at[i])
            for src, dst, sem in ((g_ref, g_buf, g_sem), (v_ref, v_buf, v_sem))
        ]

    @pl.loop(0, count)
    def _(i):
        for copy in inputs(i):
            copy.start()

    barrier = pltpu.get_barrier_semaphore()
    greet = lambda dev: pl.semaphore_signal(barrier, inc=1, device_id=dev, device_id_type=MESH)
    greet(over)
    greet(twin)
    greet((me, 1 - t))
    greet(twin[:1] + (1 - t,))
    pl.when(has_up)(lambda: greet(up))
    pl.when(has_down)(lambda: greet(down))

    def lanes_of(slot, c):
        return pl.ds(pl.multiple_of((slot * 2 + c) * LANES, LANES), LANES)

    def number(d, r):
        return (z + d) * 2 + (1 - x if r else x)

    def place(shift, d, r, i):
        return all_ref.at[rows_of(chunk(i)), lanes_of(slot_at(z, shift, d, r), core)]

    def along(d, r, i, way):
        q = number(d, r)
        return pltpu.make_async_remote_copy(
            src_ref=place(0, d, r, i), dst_ref=place(1 if way else -1, d, r, i),
            send_sem=z_send.at[way, q, i], recv_sem=recv.at[q, i],
            device_id=(down, up)[way], device_id_type=MESH)

    def across(d, r, i):
        q = number(d, r)
        return pltpu.make_async_remote_copy(
            src_ref=place(0, d, r, i), dst_ref=place(0, d, 1 - r, i),
            send_sem=x_send.at[q, i], recv_sem=recv.at[q, i], device_id=over, device_id_type=MESH)

    def to_twin(d, r, i):
        q = number(d, r)
        return pltpu.make_async_remote_copy(
            src_ref=place(0, d, r, i), dst_ref=place(0, d, r, i), send_sem=c_send.at[q, i],
            recv_sem=c_recv.at[q, i], device_id=twin, device_id_type=MESH)

    def to_panel(d, r, i):
        q, k = number(d, r), chunk(i)
        return pltpu.make_async_remote_copy(
            src_ref=place(0, d, r, i), dst_ref=panel_ref.at[:, lanes_of(slot_at(z, 0, d, r), core)],
            send_sem=y_send.at[q, k % 2], recv_sem=y_recv.at[q * 2 + core],
            device_id=(here * 2 + k % 2, 1 - t), device_id_type=MESH)

    def spread(d, r, i):
        to_twin(d, r, i).start()
        pl.when(owns & (chunk(i) // 2 == part))(lambda: to_panel(d, r, i).start())

    def piece():
        return all_ref.at[pl.ds(0, rows), pl.ds(0, LANES)]

    def landed(sem):
        pltpu.make_async_copy(piece(), piece(), sem).wait()

    def arrive(d, r, i):
        landed(recv.at[number(d, r), i])

    def straight(d):
        crossing = [2 if zz in (0, LINE - 1) else 1 for zz in range(LINE)]
        return pick(z, [count - crossing[zz + d] if 0 <= zz + d < LINE else None for zz in range(LINE)])

    def exists(d):
        return (z + d >= 0) & (z + d < LINE)

    def both_ways(d, r, i):
        pl.when(has_up)(lambda: along(d, r, i, 1).start())
        pl.when(has_down)(lambda: along(d, r, i, 0).start())

    def onward(d, r, i):
        if abs(d) == LINE - 1:
            return
        if d < 0:
            pl.when(has_up)(lambda: along(d, r, i, 1).start())
        else:
            pl.when(has_down)(lambda: along(d, r, i, 0).start())

    def flip(i):
        for copy in inputs(i):
            copy.wait()
        columns = rows_of(chunk(i))
        v = v_buf[:, columns].astype(jnp.float32)
        u = g_buf[:, columns].astype(jnp.float32) * (v / (1.0 + jnp.exp(-v)))
        all_ref[columns, lanes_of(0, core)] = u.astype(jnp.bfloat16).T

    def send_own(i):
        both_ways(0, 0, i)
        across(0, 0, i).start()
        spread(0, 0, i)

    flip(0)
    pl.semaphore_wait(barrier, jnp.where(end, 5, 6))

    @pl.loop(1, count)
    def _(i):
        flip(i)
        send_own(i - 1)

    send_own(count - 1)

    def from_line(d, i):
        @pl.when(exists(d))
        def _():
            arrive(d, 0, i)
            onward(d, 0, i)
            pl.when(i < straight(d))(lambda: across(d, 0, i).start())
            spread(d, 0, i)

    def from_cross(d, i):
        @pl.when(exists(d) & (i >= straight(d)))
        def _():
            arrive(d, 1, i)
            onward(d, 1, i)
            spread(d, 1, i)

    def relayed(d, i):
        @pl.when(exists(d) & (i < straight(d)))
        def _():
            arrive(d, 1, i)
            spread(d, 1, i)

    def neighbour(i):
        arrive(0, 1, i)
        pl.when(i >= straight(0))(lambda: both_ways(0, 1, i))
        spread(0, 1, i)

    def source(slot):
        a = pick(z, [ORDER[zz][slot][0] for zz in range(LINE)])
        r = pick(z, [ORDER[zz][slot][1] for zz in range(LINE)])
        return a * 2 + jnp.where(r == 1, 1 - x, x)

    def complete(slots):
        for slot in slots:
            q = source(slot)

            @pl.loop(0, count)
            def _(i):
                landed(c_recv.at[q, i])

            @pl.when(jnp.logical_not(owns))
            def _():
                for c in range(2):
                    landed(y_recv.at[q * 2 + c])

    def span(slots):
        return pl.ds(slots[0] * 2 * LANES, len(slots) * 2 * LANES)

    def prepare(slots):
        complete(slots)

        @pl.when(owns)
        def _():
            panel_ref[:, span(slots)] = all_ref[rows_of(me % count), span(slots)]

    def multiply(slots, k, add):
        product = nt_dot(all_ref[rows_of(k), span(slots)], panel_ref[:, span(slots)])
        if add:
            product += part_ref[rows_of(k), :]
        part_ref[rows_of(k), :] = product

    @pl.loop(0, count)
    def _(i):
        from_line(-1, i)
        from_line(1, i)
        neighbour(i)

    @pl.loop(0, count)
    def _(i):
        from_line(-2, i)
        from_line(2, i)
        from_cross(-1, i)
        from_cross(1, i)

        @pl.when(end)
        def _():
            relayed(-1, i)
            relayed(1, i)

        @pl.when(jnp.logical_not(end))
        def _():
            pl.when(i % 2 == 0)(lambda: relayed(-1, i // 2))
            pl.when(i % 2 == 1)(lambda: relayed(1, i // 2))

    prepare(FIRST)

    @pl.loop(0, count)
    def _(i):
        multiply(FIRST, i, False)
        from_line(-3, i)
        from_line(3, i)
        from_cross(-2, i)
        from_cross(2, i)

        @pl.when(end)
        def _():
            relayed(-2, i)
            relayed(2, i)

        @pl.when(jnp.logical_not(end))
        def _():
            later = (count + i) // 2
            pl.when(i % 2 == 0)(lambda: relayed(-1, later))
            pl.when(i % 2 == 1)(lambda: relayed(1, later))

    prepare(SECOND)

    @pl.loop(0, count)
    def _(i):
        multiply(SECOND, i, True)
        from_cross(-3, i)
        from_cross(3, i)

        @pl.when(end)
        def _():
            relayed(-3, i)
            relayed(3, i)

        @pl.when(jnp.logical_not(end))
        def _():
            relayed(-2, i)
            relayed(2, i)

    complete([LAST])

    @pl.loop(0, CHIPS)
    def _(q):
        away, mine = q // 2, q % 2 == x
        crossing = jnp.where((away == 0) | (away == LINE - 1), 2, 1)

        @pl.loop(0, count)
        def _(i):
            landed(c_send.at[q, i])
            pl.when(mine & ((i < count - crossing) | (away == z)))(lambda: landed(x_send.at[q, i]))
            goes = mine | (i >= count - crossing)
            pl.when(goes & has_up & (away <= z))(lambda: landed(z_send.at[1, q, i]))
            pl.when(goes & has_down & (away >= z))(lambda: landed(z_send.at[0, q, i]))

        @pl.when(owns)
        def _():
            for j in range(2):
                landed(y_send.at[q, j])


def gather(grad_hidden, gate, width, tokens):
    mine, hidden = gate.shape
    count = hidden // width
    sem = pltpu.SemaphoreType.DMA
    vmem = pl.BlockSpec(memory_space=pltpu.VMEM)
    held = hidden * tokens * 2 + width * tokens * 2 + hidden * width * 4
    return pl.pallas_call(
        functools.partial(gather_kernel, (count, width)),
        out_shape=(
            pltpu.VMEM((hidden, tokens), jnp.bfloat16),
            pltpu.VMEM((width, tokens), jnp.bfloat16),
            pltpu.VMEM((hidden, width), jnp.float32),
        ),
        in_specs=[pl.BlockSpec(memory_space=pl.ANY)] * 2,
        out_specs=(vmem, vmem, vmem),
        scratch_shapes=[
            pltpu.VMEM((mine, hidden), jnp.bfloat16),
            pltpu.VMEM((mine, hidden), jnp.bfloat16),
            sem((count,)),
            sem((count,)),
            sem((2, CHIPS, count)),
            sem((CHIPS, count)),
            sem((CHIPS, count)),
            sem((CHIPS, 2)),
            sem((CHIPS, count)),
            sem((CHIPS, count)),
            sem((2 * CHIPS,)),
        ],
        compiler_params=pltpu.CompilerParams(
            collective_id=0, has_side_effects=True, vmem_limit_bytes=VMEM_BYTES - held - 2**18
        ),
    )(grad_hidden, gate)


def finish_kernel(total, tile, depth, all_ref, panel_ref, part_ref, o_ref, b_ref, o_buf, sem):
    me, t, z, x, core = position()
    width = panel_ref.shape[0]
    count = all_ref.shape[0] // width
    lanes = pl.ds(LAST * 2 * LANES, 2 * LANES)

    for ours in (True, False):
        @pl.when((me // count == t) == ours)
        def _():
            rows = pl.ds(pl.multiple_of(me % count * width, width), width)
            b_ref[...] = all_ref[rows, lanes] if ours else panel_ref[:, lanes]

    def rows_of(i):
        return pl.ds(pl.multiple_of(i * tile, tile), tile)

    def out(i):
        slot = i % depth
        return pltpu.make_async_copy(o_buf.at[slot], o_ref.at[rows_of(i)], sem.at[slot])

    steps = o_ref.shape[0] // tile

    @pl.loop(0, steps)
    def _(i):
        pl.when(i >= depth)(lambda: out(i - depth).wait())
        product = nt_dot(all_ref[rows_of(i), lanes], b_ref[...])
        o_buf[i % depth] = (part_ref[rows_of(i), :] + product) * (1.0 / total)
        out(i).start()

    @pl.loop(steps - depth, steps)
    def _(i):
        out(i).wait()


def finish(everything, panel, part, tile, depth):
    hidden, tokens = everything.shape
    width = panel.shape[0]
    held = hidden * tokens * 2 + width * tokens * 2 + hidden * width * 4
    keep = lambda array: pltpu.with_memory_space_constraint(array, pltpu.VMEM)
    return pl.pallas_call(
        functools.partial(finish_kernel, tokens, tile, depth),
        out_shape=jax.ShapeDtypeStruct((hidden, width), jnp.float32),
        in_specs=[pl.BlockSpec(memory_space=pltpu.VMEM)] * 3,
        out_specs=pl.BlockSpec(memory_space=pl.ANY),
        scratch_shapes=[
            pltpu.VMEM((width, 2 * LANES), jnp.bfloat16),
            pltpu.VMEM((depth, tile, width), jnp.float32),
            pltpu.SemaphoreType.DMA((depth,)),
        ],
        compiler_params=pltpu.CompilerParams(vmem_limit_bytes=VMEM_BYTES - held - 2**18),
    )(keep(everything), keep(panel), keep(part))


def shards(grad_hidden, gate):
    tensor_count, data_count = lax.axis_size("tensor"), lax.axis_size("dp")
    mine, hidden = grad_hidden.shape
    width = hidden * tensor_count // data_count
    tokens = mine * data_count
    held = hidden * tokens * 2 + width * tokens * 2 + hidden * width * 4
    fits = (
        tensor_count == 2 and data_count == 4 * LINE and mine == LANES and width % LANES == 0
        and tokens & (tokens - 1) == 0 and held + 7 * 2**20 < VMEM_BYTES
    )
    if not fits:
        return plain(grad_hidden, gate)
    everything, panel, part = gather(grad_hidden, gate, width, tokens)
    return finish(everything, panel, part, width // 2, 3)


def solution(mesh):
    return jax.shard_map(
        shards,
        mesh=mesh,
        in_specs=(P("dp", "tensor"), P("dp", "tensor")),
        out_specs=P("tensor", "dp"),
        check_vma=False,
    )
```

```python
import functools

import jax
import jax.numpy as jnp
from jax import lax
from jax.experimental import pallas as pl
from jax.experimental.pallas import tpu as pltpu
from jax.sharding import PartitionSpec as P

MESH = pl.DeviceIdType.MESH
LANES = 128
LINE = 4
CHIPS = 2 * LINE
VMEM_BYTES = 67_043_328

BOTTOM = {
    0: [(0, 0), (0, 1), (1, 0), (2, 0), (1, 1), (3, 0), (2, 1), (3, 1)],
    1: [(1, 0), (1, 1), (0, 0), (2, 0), (3, 0), (0, 1), (2, 1), (3, 1)],
}
ORDER = [BOTTOM[z] if z in BOTTOM else [(LINE - 1 - a, r) for a, r in BOTTOM[LINE - 1 - z]] for z in range(LINE)]
FIRST, SECOND = range(0, 5), range(5, 7)
LAST = CHIPS - 1


def activations(grad_hidden, gate):
    return (grad_hidden.astype(jnp.float32) * jax.nn.silu(gate.astype(jnp.float32))).astype(
        jnp.bfloat16
    )


def plain(grad_hidden, gate):
    up_grad = activations(grad_hidden, gate)
    tensor_count = lax.axis_size("tensor")
    data_count = lax.axis_size("dp")
    col_width = up_grad.shape[1] * tensor_count // data_count
    ratio = data_count // tensor_count
    data_index = lax.axis_index("dp")
    owner = data_index // ratio
    offset = data_index % ratio * col_width
    contract = (((0,), (0,)), ((), ()))
    total_tokens = up_grad.shape[0] * data_count
    rows_all = lax.all_gather(up_grad, "dp", axis=0, tiled=True)
    panel = lax.dynamic_slice_in_dim(rows_all, offset, col_width, 1)
    slices = lax.all_gather(panel, "tensor", axis=1, tiled=True)
    cols_all = lax.dynamic_slice_in_dim(slices, owner * col_width, col_width, 1)
    summed = lax.dot_general(rows_all, cols_all, contract, preferred_element_type=jnp.float32)
    return summed / total_tokens


def pick(index, values):
    known = [v for v in values if v is not None]
    if all(v == known[0] for v in known):
        return jnp.int32(known[0])
    out = jnp.int32(known[-1])
    for j, v in enumerate(values):
        if v is not None and v != known[-1]:
            out = jnp.where(index == j, v, out)
    return out


def slot_at(z, shift, d, r):
    def one(zz):
        if not (0 <= zz + d < LINE and 0 <= zz + shift < LINE):
            return None
        return ORDER[zz + shift].index((zz + d, r))
    return pick(z, [one(zz) for zz in range(LINE)])


def nt_dot(a, b):
    return lax.dot_general(a, b, (((1,), (1,)), ((), ())), preferred_element_type=jnp.float32)


def position():
    me, t = lax.axis_index("dp"), lax.axis_index("tensor")
    return me, t, me // 4, me // 2 % 2, me % 2


def gather_kernel(
    dims, g_ref, v_ref, all_ref, panel_ref, part_ref, g_buf, v_buf, g_sem, v_sem,
    z_send, x_send, c_send, y_send, recv, c_recv, y_recv,
):
    count, rows = dims
    me, t, z, x, core = position()
    here = me // 2
    half = CHIPS // 2
    early = count // 2
    owns = here // half == t
    part = here % half
    end = (z == 0) | (z == LINE - 1)
    has_up, has_down = z < LINE - 1, z > 0

    up = (jnp.minimum(z + 1, LINE - 1) * 4 + x * 2 + core, t)
    down = (jnp.maximum(z - 1, 0) * 4 + x * 2 + core, t)
    over = (z * 4 + (1 - x) * 2 + core, t)
    twin = (z * 4 + x * 2 + 1 - core, t)

    def chunk(i):
        return jnp.where(t == 0, i, count - 1 - i)

    def rows_of(k):
        return pl.ds(pl.multiple_of(k * rows, rows), rows)

    def inputs(i):
        return [
            pltpu.make_async_copy(src.at[:, rows_of(chunk(i))], dst.at[i % 2], sem.at[i % 2])
            for src, dst, sem in ((g_ref, g_buf, g_sem), (v_ref, v_buf, v_sem))
        ]

    for copy in inputs(0):
        copy.start()

    barrier = pltpu.get_barrier_semaphore()
    greet = lambda dev: pl.semaphore_signal(barrier, inc=1, device_id=dev, device_id_type=MESH)
    greet(over)
    greet(twin)
    greet((me, 1 - t))
    greet(twin[:1] + (1 - t,))
    pl.when(has_up)(lambda: greet(up))
    pl.when(has_down)(lambda: greet(down))

    def lanes_of(slot, c):
        return pl.ds(pl.multiple_of((slot * 2 + c) * LANES, LANES), LANES)

    def number(d, r):
        return (z + d) * 2 + (1 - x if r else x)

    def place(shift, d, r, i):
        return all_ref.at[rows_of(chunk(i)), lanes_of(slot_at(z, shift, d, r), core)]

    def along(d, r, i, way):
        q = number(d, r)
        return pltpu.make_async_remote_copy(
            src_ref=place(0, d, r, i), dst_ref=place(1 if way else -1, d, r, i),
            send_sem=z_send.at[way, q, i], recv_sem=recv.at[q, i],
            device_id=(down, up)[way], device_id_type=MESH)

    def across(d, r, i):
        q = number(d, r)
        return pltpu.make_async_remote_copy(
            src_ref=place(0, d, r, i), dst_ref=place(0, d, 1 - r, i),
            send_sem=x_send.at[q, i], recv_sem=recv.at[q, i], device_id=over, device_id_type=MESH)

    def to_twin(d, r, i):
        q = number(d, r)
        return pltpu.make_async_remote_copy(
            src_ref=place(0, d, r, i), dst_ref=place(0, d, r, i), send_sem=c_send.at[q, i],
            recv_sem=c_recv.at[q, i], device_id=twin, device_id_type=MESH)

    def to_panel(d, r, i):
        q, k = number(d, r), chunk(i)
        return pltpu.make_async_remote_copy(
            src_ref=place(0, d, r, i), dst_ref=panel_ref.at[:, lanes_of(slot_at(z, 0, d, r), core)],
            send_sem=y_send.at[q, k % 2], recv_sem=y_recv.at[q * 2 + core],
            device_id=(here * 2 + k % 2, 1 - t), device_id_type=MESH)

    def spread(d, r, i):
        to_twin(d, r, i).start()
        pl.when(owns & (chunk(i) // 2 == part))(lambda: to_panel(d, r, i).start())

    def piece():
        return all_ref.at[pl.ds(0, rows), pl.ds(0, LANES)]

    def landed(sem):
        pltpu.make_async_copy(piece(), piece(), sem).wait()

    def arrive(d, r, i):
        landed(recv.at[number(d, r), i])

    def straight(d):
        crossing = [2 if zz in (0, LINE - 1) else 1 for zz in range(LINE)]
        return pick(z, [count - crossing[zz + d] if 0 <= zz + d < LINE else None for zz in range(LINE)])

    def exists(d):
        return (z + d >= 0) & (z + d < LINE)

    def both_ways(d, r, i):
        pl.when(has_up)(lambda: along(d, r, i, 1).start())
        pl.when(has_down)(lambda: along(d, r, i, 0).start())

    def onward(d, r, i):
        if abs(d) == LINE - 1:
            return
        if d < 0:
            pl.when(has_up)(lambda: along(d, r, i, 1).start())
        else:
            pl.when(has_down)(lambda: along(d, r, i, 0).start())

    def flip(i):
        for copy in inputs(i):
            copy.wait()
        columns = rows_of(chunk(i))
        v = v_buf[i % 2].astype(jnp.float32)
        u = g_buf[i % 2].astype(jnp.float32) * (v / (1.0 + jnp.exp(-v)))
        all_ref[columns, lanes_of(0, core)] = u.astype(jnp.bfloat16).T

    def send_own(i):
        both_ways(0, 0, i)
        across(0, 0, i).start()
        spread(0, 0, i)

    def fetch(i):
        for copy in inputs(i):
            copy.start()

    flip(0)
    fetch(1)
    pl.semaphore_wait(barrier, jnp.where(end, 5, 6))
    send_own(0)
    fetch(2)
    flip(1)

    @pl.loop(2, count)
    def _(i):
        pl.when(i + 1 < count)(lambda: fetch(i + 1))
        flip(i)
        send_own(i - 1)

    send_own(count - 1)

    def from_line(d, i):
        @pl.when(exists(d))
        def _():
            arrive(d, 0, i)
            onward(d, 0, i)
            pl.when(i < straight(d))(lambda: across(d, 0, i).start())
            spread(d, 0, i)

    def from_cross(d, i):
        @pl.when(exists(d) & (i >= straight(d)))
        def _():
            arrive(d, 1, i)
            onward(d, 1, i)
            spread(d, 1, i)

    def relayed(d, i):
        @pl.when(exists(d) & (i < straight(d)))
        def _():
            arrive(d, 1, i)
            spread(d, 1, i)

    def neighbour(i):
        arrive(0, 1, i)
        pl.when(i >= straight(0))(lambda: both_ways(0, 1, i))
        spread(0, 1, i)

    def source(slot):
        a = pick(z, [ORDER[zz][slot][0] for zz in range(LINE)])
        r = pick(z, [ORDER[zz][slot][1] for zz in range(LINE)])
        return a * 2 + jnp.where(r == 1, 1 - x, x)

    def span(slots):
        return pl.ds(slots[0] * 2 * LANES, len(slots) * 2 * LANES)

    def twin_sent(slots, i):
        for slot in slots:
            landed(c_recv.at[source(slot), i])

    def all_twin_sent(slots, first, last):
        @pl.loop(first, last)
        def _(i):
            twin_sent(slots, i)

    def panel_arrived(slots):
        for slot in slots:
            for c in range(2):
                landed(y_recv.at[source(slot) * 2 + c])

    def columns(slots):
        pl.when(jnp.logical_not(owns))(lambda: panel_arrived(slots))

        @pl.when(owns)
        def _():
            panel_ref[:, span(slots)] = all_ref[rows_of(me % count), span(slots)]

    def multiply(slots, k, add):
        product = nt_dot(all_ref[rows_of(k), span(slots)], panel_ref[:, span(slots)])
        if add:
            product += part_ref[rows_of(k), :]
        part_ref[rows_of(k), :] = product

    @pl.loop(0, count)
    def _(i):
        from_line(-1, i)
        from_line(1, i)
        neighbour(i)

    @pl.loop(0, count)
    def _(i):
        from_line(-2, i)
        from_line(2, i)
        from_cross(-1, i)
        from_cross(1, i)

        @pl.when(end)
        def _():
            relayed(-1, i)
            relayed(1, i)

        @pl.when(jnp.logical_not(end))
        def _():
            pl.when(i % 2 == 0)(lambda: relayed(-1, i // 2))
            pl.when(i % 2 == 1)(lambda: relayed(1, i // 2))

    all_twin_sent(FIRST, 0, count)
    columns(FIRST)

    @pl.loop(0, count)
    def _(i):
        multiply(FIRST, chunk(i), False)
        from_line(-3, i)
        from_line(3, i)
        from_cross(-2, i)
        from_cross(2, i)

        @pl.when(end)
        def _():
            relayed(-2, i)
            relayed(2, i)

        @pl.when(jnp.logical_not(end))
        def _():
            later = (count + i) // 2
            pl.when(i % 2 == 0)(lambda: relayed(-1, later))
            pl.when(i % 2 == 1)(lambda: relayed(1, later))

        @pl.when(end & (i == early))
        def _():
            all_twin_sent(SECOND, 0, early)
            columns(SECOND)

        @pl.when(end & (i >= early))
        def _():
            multiply(SECOND, chunk(i - early), True)

    @pl.when(jnp.logical_not(end))
    def _():
        all_twin_sent(SECOND, 0, count)
        columns(SECOND)

    def sent(nearby):
        @pl.loop(0, CHIPS)
        def _(q):
            away, mine = q // 2, q % 2 == x
            crossing = jnp.where((away == 0) | (away == LINE - 1), 2, 1)

            @pl.when((jnp.abs(away - z) <= 1) == nearby)
            def _():
                @pl.loop(0, count)
                def _(i):
                    landed(c_send.at[q, i])
                    pl.when(mine & ((i < count - crossing) | (away == z)))(lambda: landed(x_send.at[q, i]))
                    goes = mine | (i >= count - crossing)
                    pl.when(goes & has_up & (away <= z))(lambda: landed(z_send.at[1, q, i]))
                    pl.when(goes & has_down & (away >= z))(lambda: landed(z_send.at[0, q, i]))

                @pl.when(owns)
                def _():
                    for j in range(2):
                        landed(y_send.at[q, j])

    @pl.loop(0, count)
    def _(i):
        from_cross(-3, i)
        from_cross(3, i)

        @pl.when(end)
        def _():
            relayed(-3, i)
            relayed(3, i)

        @pl.when(jnp.logical_not(end))
        def _():
            relayed(-2, i)
            relayed(2, i)

        later = jnp.where(end, i + count - early, i)

        @pl.when(later < count)
        def _():
            pl.when(end)(lambda: twin_sent(SECOND, later))
            multiply(SECOND, chunk(later), True)

        pl.when(i == early)(lambda: sent(True))

    all_twin_sent([LAST], 0, count)
    pl.when(jnp.logical_not(owns))(lambda: panel_arrived([LAST]))
    sent(False)


def gather(grad_hidden, gate, width, tokens):
    mine, hidden = gate.shape
    count = hidden // width
    sem = pltpu.SemaphoreType.DMA
    vmem = pl.BlockSpec(memory_space=pltpu.VMEM)
    held = hidden * tokens * 2 + width * tokens * 2 + hidden * width * 4
    return pl.pallas_call(
        functools.partial(gather_kernel, (count, width)),
        out_shape=(
            pltpu.VMEM((hidden, tokens), jnp.bfloat16),
            pltpu.VMEM((width, tokens), jnp.bfloat16),
            pltpu.VMEM((hidden, width), jnp.float32),
        ),
        in_specs=[pl.BlockSpec(memory_space=pl.ANY)] * 2,
        out_specs=(vmem, vmem, vmem),
        scratch_shapes=[
            pltpu.VMEM((2, mine, width), jnp.bfloat16),
            pltpu.VMEM((2, mine, width), jnp.bfloat16),
            sem((2,)),
            sem((2,)),
            sem((2, CHIPS, count)),
            sem((CHIPS, count)),
            sem((CHIPS, count)),
            sem((CHIPS, 2)),
            sem((CHIPS, count)),
            sem((CHIPS, count)),
            sem((2 * CHIPS,)),
        ],
        compiler_params=pltpu.CompilerParams(
            collective_id=0, has_side_effects=True, vmem_limit_bytes=VMEM_BYTES - held - 2**18
        ),
    )(grad_hidden, gate)


def finish_kernel(total, tile, all_ref, panel_ref, _, o_ref, part_ref, b_ref, sem):
    me, t, z, x, core = position()
    width = panel_ref.shape[0]
    count = all_ref.shape[0] // width
    lanes = pl.ds(LAST * 2 * LANES, 2 * LANES)

    for ours in (True, False):
        @pl.when((me // count == t) == ours)
        def _():
            rows = pl.ds(pl.multiple_of(me % count * width, width), width)
            b_ref[...] = all_ref[rows, lanes] if ours else panel_ref[:, lanes]

    def rows_of(i):
        return pl.ds(pl.multiple_of(i * tile, tile), tile)

    def out(i):
        return pltpu.make_async_copy(part_ref.at[rows_of(i)], o_ref.at[rows_of(i)], sem.at[i])

    steps = o_ref.shape[0] // tile

    @pl.loop(0, steps)
    def _(i):
        product = nt_dot(all_ref[rows_of(i), lanes], b_ref[...])
        part_ref[rows_of(i), :] = (part_ref[rows_of(i), :] + product) * (1.0 / total)
        out(i).start()

    @pl.loop(0, steps)
    def _(i):
        out(i).wait()


def finish(everything, panel, part, tile):
    hidden, tokens = everything.shape
    width = panel.shape[0]
    held = hidden * tokens * 2 + width * tokens * 2 + hidden * width * 4
    keep = lambda array: pltpu.with_memory_space_constraint(array, pltpu.VMEM)
    vmem = pl.BlockSpec(memory_space=pltpu.VMEM)
    return pl.pallas_call(
        functools.partial(finish_kernel, tokens, tile),
        out_shape=(
            jax.ShapeDtypeStruct((hidden, width), jnp.float32),
            pltpu.VMEM((hidden, width), jnp.float32),
        ),
        in_specs=[vmem] * 3,
        out_specs=(pl.BlockSpec(memory_space=pl.ANY), vmem),
        input_output_aliases={2: 1},
        scratch_shapes=[
            pltpu.VMEM((width, 2 * LANES), jnp.bfloat16),
            pltpu.SemaphoreType.DMA((hidden // tile,)),
        ],
        compiler_params=pltpu.CompilerParams(vmem_limit_bytes=VMEM_BYTES - held - 2**18),
    )(keep(everything), keep(panel), keep(part))[0]


def shards(grad_hidden, gate):
    tensor_count, data_count = lax.axis_size("tensor"), lax.axis_size("dp")
    mine, hidden = grad_hidden.shape
    width = hidden * tensor_count // data_count
    tokens = mine * data_count
    held = hidden * tokens * 2 + width * tokens * 2 + hidden * width * 4
    fits = (
        tensor_count == 2 and data_count == 4 * LINE and mine == LANES and width % LANES == 0
        and tokens & (tokens - 1) == 0 and held + 7 * 2**20 < VMEM_BYTES
    )
    if not fits:
        return plain(grad_hidden, gate)
    everything, panel, part = gather(grad_hidden, gate, width, tokens)
    return finish(everything, panel, part, width // 2)


def solution(mesh):
    return jax.shard_map(
        shards,
        mesh=mesh,
        in_specs=(P("dp", "tensor"), P("dp", "tensor")),
        out_specs=P("tensor", "dp"),
        check_vma=False,
    )
```

```python
import functools

import jax
import jax.numpy as jnp
from jax import lax
from jax.experimental import pallas as pl
from jax.experimental.pallas import tpu as pltpu
from jax.sharding import PartitionSpec as P

MESH = pl.DeviceIdType.MESH
LANES = 128
LINE = 4
CHIPS = 2 * LINE
VMEM_BYTES = 67_043_328

BOTTOM = {
    0: [(0, 0), (0, 1), (1, 0), (2, 0), (1, 1), (3, 0), (2, 1), (3, 1)],
    1: [(1, 0), (1, 1), (0, 0), (2, 0), (3, 0), (0, 1), (2, 1), (3, 1)],
}
ORDER = [BOTTOM[z] if z in BOTTOM else [(LINE - 1 - a, r) for a, r in BOTTOM[LINE - 1 - z]] for z in range(LINE)]
FIRST, SECOND = range(0, 5), range(5, 7)
LAST = CHIPS - 1
CROSSING = [2 if z in (0, LINE - 1) else 1 for z in range(LINE)]


def activations(grad_hidden, gate):
    return (grad_hidden.astype(jnp.float32) * jax.nn.silu(gate.astype(jnp.float32))).astype(
        jnp.bfloat16
    )


def plain(grad_hidden, gate):
    up_grad = activations(grad_hidden, gate)
    tensor_count = lax.axis_size("tensor")
    data_count = lax.axis_size("dp")
    col_width = up_grad.shape[1] * tensor_count // data_count
    ratio = data_count // tensor_count
    data_index = lax.axis_index("dp")
    owner = data_index // ratio
    offset = data_index % ratio * col_width
    contract = (((0,), (0,)), ((), ()))
    total_tokens = up_grad.shape[0] * data_count
    rows_all = lax.all_gather(up_grad, "dp", axis=0, tiled=True)
    panel = lax.dynamic_slice_in_dim(rows_all, offset, col_width, 1)
    slices = lax.all_gather(panel, "tensor", axis=1, tiled=True)
    cols_all = lax.dynamic_slice_in_dim(slices, owner * col_width, col_width, 1)
    summed = lax.dot_general(rows_all, cols_all, contract, preferred_element_type=jnp.float32)
    return summed / total_tokens


def pick(index, values):
    known = [v for v in values if v is not None]
    if all(v == known[0] for v in known):
        return jnp.int32(known[0])
    out = jnp.int32(known[-1])
    for j, v in enumerate(values):
        if v is not None and v != known[-1]:
            out = jnp.where(index == j, v, out)
    return out


def slot_at(z, shift, d, r):
    def one(zz):
        if not (0 <= zz + d < LINE and 0 <= zz + shift < LINE):
            return None
        return ORDER[zz + shift].index((zz + d, r))
    return pick(z, [one(zz) for zz in range(LINE)])


def nt_dot(a, b):
    return lax.dot_general(a, b, (((1,), (1,)), ((), ())), preferred_element_type=jnp.float32)


def position():
    me, t = lax.axis_index("dp"), lax.axis_index("tensor")
    return me, t, me // 4, me // 2 % 2, me % 2


def gather_kernel(
    dims, g_ref, v_ref, all_ref, panel_ref, part_ref, g_buf, v_buf, g_sem, v_sem,
    z_send, x_send, c_send, y_send, recv, c_recv, y_recv,
):
    count, rows = dims
    me, t, z, x, core = position()
    here = me // 2
    half = CHIPS // 2
    early = count // 2
    owns = here // half == t
    part = here % half
    end = (z == 0) | (z == LINE - 1)
    has_up, has_down = z < LINE - 1, z > 0

    up = (jnp.minimum(z + 1, LINE - 1) * 4 + x * 2 + core, t)
    down = (jnp.maximum(z - 1, 0) * 4 + x * 2 + core, t)
    over = (z * 4 + (1 - x) * 2 + core, t)
    twin = (z * 4 + x * 2 + 1 - core, t)

    def chunk(i):
        return jnp.where(t == 0, i, count - 1 - i)

    def rows_of(k):
        return pl.ds(pl.multiple_of(k * rows, rows), rows)

    def inputs(i):
        return [
            pltpu.make_async_copy(src.at[:, rows_of(chunk(i))], dst.at[i % 2], sem.at[i % 2])
            for src, dst, sem in ((g_ref, g_buf, g_sem), (v_ref, v_buf, v_sem))
        ]

    for copy in inputs(0):
        copy.start()

    barrier = pltpu.get_barrier_semaphore()
    greet = lambda dev: pl.semaphore_signal(barrier, inc=1, device_id=dev, device_id_type=MESH)
    greet(over)
    greet(twin)
    greet((me, 1 - t))
    greet(twin[:1] + (1 - t,))
    pl.when(has_up)(lambda: greet(up))
    pl.when(has_down)(lambda: greet(down))

    def lanes_of(slot, c):
        return pl.ds(pl.multiple_of((slot * 2 + c) * LANES, LANES), LANES)

    def number(d, r):
        return (z + d) * 2 + (1 - x if r else x)

    def place(shift, d, r, i):
        return all_ref.at[rows_of(chunk(i)), lanes_of(slot_at(z, shift, d, r), core)]

    def along(d, r, i, way):
        q = number(d, r)
        return pltpu.make_async_remote_copy(
            src_ref=place(0, d, r, i), dst_ref=place(1 if way else -1, d, r, i),
            send_sem=z_send.at[way], recv_sem=recv.at[q, i],
            device_id=(down, up)[way], device_id_type=MESH)

    def across(d, r, i):
        q = number(d, r)
        return pltpu.make_async_remote_copy(
            src_ref=place(0, d, r, i), dst_ref=place(0, d, 1 - r, i),
            send_sem=x_send, recv_sem=recv.at[q, i], device_id=over, device_id_type=MESH)

    def to_twin(d, r, i):
        slot = slot_at(z, 0, d, r)
        later = 2 + jnp.maximum(i - early + 1, 0)
        index = jnp.where(slot < SECOND[0], 0, jnp.where(slot == LAST, 1, later))
        return pltpu.make_async_remote_copy(
            src_ref=place(0, d, r, i), dst_ref=place(0, d, r, i), send_sem=c_send,
            recv_sem=c_recv.at[index], device_id=twin, device_id_type=MESH)

    def to_panel(d, r, i):
        k, slot = chunk(i), slot_at(z, 0, d, r)
        index = jnp.where(slot < SECOND[0], 0, jnp.where(slot == LAST, 2, 1))
        return pltpu.make_async_remote_copy(
            src_ref=place(0, d, r, i), dst_ref=panel_ref.at[:, lanes_of(slot, core)],
            send_sem=y_send, recv_sem=y_recv.at[index],
            device_id=(here * 2 + k % 2, 1 - t), device_id_type=MESH)

    def spread(d, r, i):
        to_twin(d, r, i).start()
        pl.when(owns & (chunk(i) // 2 == part))(lambda: to_panel(d, r, i).start())

    def landed(sem, chunks=1):
        piece = all_ref.at[pl.ds(0, chunks * rows // 8), pl.ds(0, 8 * LANES)]
        pltpu.make_async_copy(piece, piece, sem).wait()

    def arrive(d, r, i):
        landed(recv.at[number(d, r), i])

    def straight(d):
        return pick(z, [count - CROSSING[zz + d] if 0 <= zz + d < LINE else None for zz in range(LINE)])

    def exists(d):
        return (z + d >= 0) & (z + d < LINE)

    def both_ways(d, r, i):
        pl.when(has_up)(lambda: along(d, r, i, 1).start())
        pl.when(has_down)(lambda: along(d, r, i, 0).start())

    def onward(d, r, i):
        if abs(d) == LINE - 1:
            return
        if d < 0:
            pl.when(has_up)(lambda: along(d, r, i, 1).start())
        else:
            pl.when(has_down)(lambda: along(d, r, i, 0).start())

    def flip(i):
        for copy in inputs(i):
            copy.wait()
        columns = rows_of(chunk(i))
        v = v_buf[i % 2].astype(jnp.float32)
        u = g_buf[i % 2].astype(jnp.float32) * (v / (1.0 + jnp.exp(-v)))
        all_ref[columns, lanes_of(0, core)] = u.astype(jnp.bfloat16).T

    def send_own(i):
        both_ways(0, 0, i)
        across(0, 0, i).start()
        spread(0, 0, i)

    def fetch(i):
        for copy in inputs(i):
            copy.start()

    flip(0)
    fetch(1)
    pl.semaphore_wait(barrier, jnp.where(end, 5, 6))
    send_own(0)
    fetch(2)
    flip(1)

    @pl.loop(2, count)
    def _(i):
        pl.when(i + 1 < count)(lambda: fetch(i + 1))
        flip(i)
        send_own(i - 1)

    send_own(count - 1)

    def from_line(d, i):
        @pl.when(exists(d))
        def _():
            arrive(d, 0, i)
            onward(d, 0, i)
            pl.when(i < straight(d))(lambda: across(d, 0, i).start())
            spread(d, 0, i)

    def from_cross(d, i):
        @pl.when(exists(d) & (i >= straight(d)))
        def _():
            arrive(d, 1, i)
            onward(d, 1, i)
            spread(d, 1, i)

    def relayed(d, i):
        @pl.when(exists(d) & (i < straight(d)))
        def _():
            arrive(d, 1, i)
            spread(d, 1, i)

    def neighbour(i):
        arrive(0, 1, i)
        pl.when(i >= straight(0))(lambda: both_ways(0, 1, i))
        spread(0, 1, i)

    def span(slots):
        return pl.ds(slots[0] * 2 * LANES, len(slots) * 2 * LANES)

    def columns(slots, group):
        pl.when(jnp.logical_not(owns))(lambda: landed(y_recv.at[group], 2 * len(slots)))

        @pl.when(owns)
        def _():
            panel_ref[:, span(slots)] = all_ref[rows_of(me % count), span(slots)]

    def multiply(slots, k, add):
        product = nt_dot(all_ref[rows_of(k), span(slots)], panel_ref[:, span(slots)])
        if add:
            product += part_ref[rows_of(k), :]
        part_ref[rows_of(k), :] = product

    @pl.loop(0, count)
    def _(i):
        from_line(-1, i)
        from_line(1, i)
        neighbour(i)

    @pl.loop(0, count)
    def _(i):
        from_line(-2, i)
        from_line(2, i)
        from_cross(-1, i)
        from_cross(1, i)

        @pl.when(end)
        def _():
            relayed(-1, i)
            relayed(1, i)

        @pl.when(jnp.logical_not(end))
        def _():
            pl.when(i % 2 == 0)(lambda: relayed(-1, i // 2))
            pl.when(i % 2 == 1)(lambda: relayed(1, i // 2))

    landed(c_recv.at[0], len(FIRST) * count)
    columns(FIRST, 0)

    @pl.loop(0, count)
    def _(i):
        multiply(FIRST, chunk(i), False)
        from_line(-3, i)
        from_line(3, i)
        from_cross(-2, i)
        from_cross(2, i)

        @pl.when(end)
        def _():
            relayed(-2, i)
            relayed(2, i)

        @pl.when(jnp.logical_not(end))
        def _():
            later = (count + i) // 2
            pl.when(i % 2 == 0)(lambda: relayed(-1, later))
            pl.when(i % 2 == 1)(lambda: relayed(1, later))

        @pl.when(end & (i == early))
        def _():
            landed(c_recv.at[2], len(SECOND) * early)
            columns(SECOND, 1)

        @pl.when(end & (i >= early))
        def _():
            multiply(SECOND, chunk(i - early), True)

    @pl.when(jnp.logical_not(end))
    def _():
        landed(c_recv.at[2], len(SECOND) * early)
        for i in range(early, count):
            landed(c_recv.at[3 + i - early], len(SECOND))
        columns(SECOND, 1)

    @pl.loop(0, count)
    def _(i):
        from_cross(-3, i)
        from_cross(3, i)

        @pl.when(end)
        def _():
            relayed(-3, i)
            relayed(3, i)

        @pl.when(jnp.logical_not(end))
        def _():
            relayed(-2, i)
            relayed(2, i)

        later = jnp.where(end, i + count - early, i)

        @pl.when(later < count)
        def _():
            pl.when(end)(lambda: landed(c_recv.at[3 + i], len(SECOND)))
            multiply(SECOND, chunk(later), True)

    landed(c_recv.at[1], count)
    pl.when(jnp.logical_not(owns))(lambda: landed(y_recv.at[2], 2))
    landed(c_send, CHIPS * count)
    pl.when(owns)(lambda: landed(y_send, 2 * CHIPS))
    for zz in range(LINE):
        @pl.when(z == zz)
        def _():
            landed(x_send, CROSSING[zz] + sum(count - c for c in CROSSING))
            if zz < LINE - 1:
                landed(z_send.at[1], sum(count + c for c in CROSSING[:zz + 1]))
            if zz > 0:
                landed(z_send.at[0], sum(count + c for c in CROSSING[zz:]))


def gather(grad_hidden, gate, width, tokens):
    mine, hidden = gate.shape
    count = hidden // width
    sem = pltpu.SemaphoreType.DMA
    vmem = pl.BlockSpec(memory_space=pltpu.VMEM)
    held = hidden * tokens * 2 + width * tokens * 2 + hidden * width * 4
    return pl.pallas_call(
        functools.partial(gather_kernel, (count, width)),
        out_shape=(
            pltpu.VMEM((hidden, tokens), jnp.bfloat16),
            pltpu.VMEM((width, tokens), jnp.bfloat16),
            pltpu.VMEM((hidden, width), jnp.float32),
        ),
        in_specs=[pl.BlockSpec(memory_space=pl.ANY)] * 2,
        out_specs=(vmem, vmem, vmem),
        scratch_shapes=[
            pltpu.VMEM((2, mine, width), jnp.bfloat16),
            pltpu.VMEM((2, mine, width), jnp.bfloat16),
            sem((2,)),
            sem((2,)),
            sem((2,)),
            sem(()),
            sem(()),
            sem(()),
            sem((CHIPS, count)),
            sem((3 + count - count // 2,)),
            sem((3,)),
        ],
        compiler_params=pltpu.CompilerParams(
            collective_id=0, has_side_effects=True, vmem_limit_bytes=VMEM_BYTES - held - 2**18
        ),
    )(grad_hidden, gate)


def finish_kernel(total, tile, all_ref, panel_ref, _, o_ref, part_ref, b_ref, sem):
    me, t, z, x, core = position()
    width = panel_ref.shape[0]
    count = all_ref.shape[0] // width
    lanes = pl.ds(LAST * 2 * LANES, 2 * LANES)

    for ours in (True, False):
        @pl.when((me // count == t) == ours)
        def _():
            rows = pl.ds(pl.multiple_of(me % count * width, width), width)
            b_ref[...] = all_ref[rows, lanes] if ours else panel_ref[:, lanes]

    def rows_of(i):
        return pl.ds(pl.multiple_of(i * tile, tile), tile)

    def out(i):
        return pltpu.make_async_copy(part_ref.at[rows_of(i)], o_ref.at[rows_of(i)], sem.at[i])

    steps = o_ref.shape[0] // tile

    @pl.loop(0, steps)
    def _(i):
        product = nt_dot(all_ref[rows_of(i), lanes], b_ref[...])
        part_ref[rows_of(i), :] = (part_ref[rows_of(i), :] + product) * (1.0 / total)
        out(i).start()

    @pl.loop(0, steps)
    def _(i):
        out(i).wait()


def finish(everything, panel, part, tile):
    hidden, tokens = everything.shape
    width = panel.shape[0]
    held = hidden * tokens * 2 + width * tokens * 2 + hidden * width * 4
    keep = lambda array: pltpu.with_memory_space_constraint(array, pltpu.VMEM)
    vmem = pl.BlockSpec(memory_space=pltpu.VMEM)
    return pl.pallas_call(
        functools.partial(finish_kernel, tokens, tile),
        out_shape=(
            jax.ShapeDtypeStruct((hidden, width), jnp.float32),
            pltpu.VMEM((hidden, width), jnp.float32),
        ),
        in_specs=[vmem] * 3,
        out_specs=(pl.BlockSpec(memory_space=pl.ANY), vmem),
        input_output_aliases={2: 1},
        scratch_shapes=[
            pltpu.VMEM((width, 2 * LANES), jnp.bfloat16),
            pltpu.SemaphoreType.DMA((hidden // tile,)),
        ],
        compiler_params=pltpu.CompilerParams(vmem_limit_bytes=VMEM_BYTES - held - 2**18),
    )(keep(everything), keep(panel), keep(part))[0]


def shards(grad_hidden, gate):
    tensor_count, data_count = lax.axis_size("tensor"), lax.axis_size("dp")
    mine, hidden = grad_hidden.shape
    width = hidden * tensor_count // data_count
    tokens = mine * data_count
    held = hidden * tokens * 2 + width * tokens * 2 + hidden * width * 4
    fits = (
        tensor_count == 2 and data_count == 4 * LINE and mine == LANES and width % LANES == 0
        and tokens & (tokens - 1) == 0 and held + 7 * 2**20 < VMEM_BYTES
    )
    if not fits:
        return plain(grad_hidden, gate)
    everything, panel, part = gather(grad_hidden, gate, width, tokens)
    return finish(everything, panel, part, width // 2)


def solution(mesh):
    return jax.shard_map(
        shards,
        mesh=mesh,
        in_specs=(P("dp", "tensor"), P("dp", "tensor")),
        out_specs=P("tensor", "dp"),
        check_vma=False,
    )
```

```python
import functools

import jax
import jax.numpy as jnp
from jax import lax
from jax.experimental import pallas as pl
from jax.experimental.pallas import tpu as pltpu
from jax.sharding import PartitionSpec as P

MESH = pl.DeviceIdType.MESH
LANES = 128
LINE = 4
CHIPS = 2 * LINE
VMEM_BYTES = 67_043_328

BOTTOM = {
    0: [(0, 0), (0, 1), (1, 0), (2, 0), (1, 1), (3, 0), (2, 1), (3, 1)],
    1: [(1, 0), (1, 1), (0, 0), (2, 0), (3, 0), (0, 1), (2, 1), (3, 1)],
}
ORDER = [BOTTOM[z] if z in BOTTOM else [(LINE - 1 - a, r) for a, r in BOTTOM[LINE - 1 - z]] for z in range(LINE)]
FIRST, SECOND = range(0, 5), range(5, 7)
LAST = CHIPS - 1
CROSSING = [2 if z in (0, LINE - 1) else 1 for z in range(LINE)]


def activations(grad_hidden, gate):
    return (grad_hidden.astype(jnp.float32) * jax.nn.silu(gate.astype(jnp.float32))).astype(
        jnp.bfloat16
    )


def plain(grad_hidden, gate):
    up_grad = activations(grad_hidden, gate)
    tensor_count = lax.axis_size("tensor")
    data_count = lax.axis_size("dp")
    col_width = up_grad.shape[1] * tensor_count // data_count
    ratio = data_count // tensor_count
    data_index = lax.axis_index("dp")
    owner = data_index // ratio
    offset = data_index % ratio * col_width
    contract = (((0,), (0,)), ((), ()))
    total_tokens = up_grad.shape[0] * data_count
    rows_all = lax.all_gather(up_grad, "dp", axis=0, tiled=True)
    panel = lax.dynamic_slice_in_dim(rows_all, offset, col_width, 1)
    slices = lax.all_gather(panel, "tensor", axis=1, tiled=True)
    cols_all = lax.dynamic_slice_in_dim(slices, owner * col_width, col_width, 1)
    summed = lax.dot_general(rows_all, cols_all, contract, preferred_element_type=jnp.float32)
    return summed / total_tokens


def pick(index, values):
    known = [v for v in values if v is not None]
    if all(v == known[0] for v in known):
        return jnp.int32(known[0])
    out = jnp.int32(known[-1])
    for j, v in enumerate(values):
        if v is not None and v != known[-1]:
            out = jnp.where(index == j, v, out)
    return out


def slot_at(z, shift, d, r):
    def one(zz):
        if not (0 <= zz + d < LINE and 0 <= zz + shift < LINE):
            return None
        return ORDER[zz + shift].index((zz + d, r))
    return pick(z, [one(zz) for zz in range(LINE)])


def nt_dot(a, b):
    return lax.dot_general(a, b, (((1,), (1,)), ((), ())), preferred_element_type=jnp.float32)


def position():
    me, t = lax.axis_index("dp"), lax.axis_index("tensor")
    return me, t, me // 4, me // 2 % 2, me % 2


def gather_kernel(
    dims, g_ref, v_ref, all_ref, panel_ref, part_ref, g_buf, v_buf, g_sem, v_sem,
    z_send, x_send, c_send, y_send, recv, c_recv, y_recv,
):
    count, rows = dims
    me, t, z, x, core = position()
    here = me // 2
    half = CHIPS // 2
    early = count // 2
    owns = here // half == t
    part = here % half
    end = (z == 0) | (z == LINE - 1)
    has_up, has_down = z < LINE - 1, z > 0

    up = (jnp.minimum(z + 1, LINE - 1) * 4 + x * 2 + core, t)
    down = (jnp.maximum(z - 1, 0) * 4 + x * 2 + core, t)
    over = (z * 4 + (1 - x) * 2 + core, t)
    twin = (z * 4 + x * 2 + 1 - core, t)

    def chunk(i):
        return jnp.where(t == 0, i, count - 1 - i)

    def rows_of(k):
        return pl.ds(pl.multiple_of(k * rows, rows), rows)

    def inputs(i):
        return [
            pltpu.make_async_copy(src.at[:, rows_of(chunk(i))], dst.at[i % 2], sem.at[i % 2])
            for src, dst, sem in ((g_ref, g_buf, g_sem), (v_ref, v_buf, v_sem))
        ]

    for copy in inputs(0):
        copy.start()

    barrier = pltpu.get_barrier_semaphore()
    greet = lambda dev: pl.semaphore_signal(barrier, inc=1, device_id=dev, device_id_type=MESH)
    greet(over)
    greet(twin)
    greet((me, 1 - t))
    greet(twin[:1] + (1 - t,))
    pl.when(has_up)(lambda: greet(up))
    pl.when(has_down)(lambda: greet(down))

    def lanes_of(slot, c):
        return pl.ds(pl.multiple_of((slot * 2 + c) * LANES, LANES), LANES)

    def number(d, r):
        return (z + d) * 2 + (1 - x if r else x)

    def place(shift, d, r, i):
        return all_ref.at[rows_of(chunk(i)), lanes_of(slot_at(z, shift, d, r), core)]

    def along(d, r, i, way):
        q = number(d, r)
        return pltpu.make_async_remote_copy(
            src_ref=place(0, d, r, i), dst_ref=place(1 if way else -1, d, r, i),
            send_sem=z_send.at[way], recv_sem=recv.at[q, i],
            device_id=(down, up)[way], device_id_type=MESH)

    def across(d, r, i):
        q = number(d, r)
        return pltpu.make_async_remote_copy(
            src_ref=place(0, d, r, i), dst_ref=place(0, d, 1 - r, i),
            send_sem=x_send, recv_sem=recv.at[q, i], device_id=over, device_id_type=MESH)

    def to_twin(d, r, i):
        slot = slot_at(z, 0, d, r)
        later = 2 + jnp.maximum(i - early + 1, 0)
        index = jnp.where(slot < SECOND[0], 0, jnp.where(slot == LAST, 1, later))
        return pltpu.make_async_remote_copy(
            src_ref=place(0, d, r, i), dst_ref=place(0, d, r, i), send_sem=c_send,
            recv_sem=c_recv.at[index], device_id=twin, device_id_type=MESH)

    def to_panel(d, r, i):
        k, slot = chunk(i), slot_at(z, 0, d, r)
        index = jnp.where(slot < SECOND[0], 0, jnp.where(slot == LAST, 2, 1))
        return pltpu.make_async_remote_copy(
            src_ref=place(0, d, r, i), dst_ref=panel_ref.at[:, lanes_of(slot, core)],
            send_sem=y_send, recv_sem=y_recv.at[index],
            device_id=(here * 2 + k % 2, 1 - t), device_id_type=MESH)

    def spread(d, r, i):
        to_twin(d, r, i).start()
        pl.when(owns & (chunk(i) // 2 == part))(lambda: to_panel(d, r, i).start())

    def landed(sem, chunks=1):
        piece = all_ref.at[pl.ds(0, chunks * rows // 8), pl.ds(0, 8 * LANES)]
        pltpu.make_async_copy(piece, piece, sem).wait()

    def arrive(d, r, i):
        landed(recv.at[number(d, r), i])

    def straight(d):
        return pick(z, [count - CROSSING[zz + d] if 0 <= zz + d < LINE else None for zz in range(LINE)])

    def exists(d):
        return (z + d >= 0) & (z + d < LINE)

    def both_ways(d, r, i):
        pl.when(has_up)(lambda: along(d, r, i, 1).start())
        pl.when(has_down)(lambda: along(d, r, i, 0).start())

    def onward(d, r, i):
        if abs(d) == LINE - 1:
            return
        if d < 0:
            pl.when(has_up)(lambda: along(d, r, i, 1).start())
        else:
            pl.when(has_down)(lambda: along(d, r, i, 0).start())

    def flip(i):
        for copy in inputs(i):
            copy.wait()
        columns = rows_of(chunk(i))
        v = v_buf[i % 2].astype(jnp.float32)
        u = g_buf[i % 2].astype(jnp.float32) * (v / (1.0 + jnp.exp(-v)))
        all_ref[columns, lanes_of(0, core)] = u.astype(jnp.bfloat16).T

    def send_own(i):
        both_ways(0, 0, i)
        across(0, 0, i).start()
        spread(0, 0, i)

    def fetch(i):
        for copy in inputs(i):
            copy.start()

    flip(0)
    fetch(1)
    pl.semaphore_wait(barrier, jnp.where(end, 5, 6))
    send_own(0)
    fetch(2)
    flip(1)

    @pl.loop(2, count)
    def _(i):
        pl.when(i + 1 < count)(lambda: fetch(i + 1))
        flip(i)
        send_own(i - 1)

    send_own(count - 1)

    def from_line(d, i):
        @pl.when(exists(d))
        def _():
            arrive(d, 0, i)
            onward(d, 0, i)
            pl.when(i < straight(d))(lambda: across(d, 0, i).start())
            spread(d, 0, i)

    def from_cross(d, i):
        @pl.when(exists(d) & (i >= straight(d)))
        def _():
            arrive(d, 1, i)
            onward(d, 1, i)
            spread(d, 1, i)

    def relayed(d, i):
        @pl.when(exists(d) & (i < straight(d)))
        def _():
            arrive(d, 1, i)
            spread(d, 1, i)

    def neighbour(i):
        arrive(0, 1, i)
        pl.when(i >= straight(0))(lambda: both_ways(0, 1, i))
        spread(0, 1, i)

    def span(slots):
        return pl.ds(slots[0] * 2 * LANES, len(slots) * 2 * LANES)

    def columns(slots, group):
        pl.when(jnp.logical_not(owns))(lambda: landed(y_recv.at[group], 2 * len(slots)))

        @pl.when(owns)
        def _():
            panel_ref[:, span(slots)] = all_ref[rows_of(me % count), span(slots)]

    def multiply(slots, k, add):
        product = nt_dot(all_ref[rows_of(k), span(slots)], panel_ref[:, span(slots)])
        if add:
            product += part_ref[rows_of(k), :]
        part_ref[rows_of(k), :] = product

    @pl.loop(0, count)
    def _(i):
        from_line(-1, i)
        from_line(1, i)
        neighbour(i)

    @pl.loop(0, count)
    def _(i):
        from_line(-2, i)
        from_line(2, i)
        from_cross(-1, i)
        from_cross(1, i)

        @pl.when(end)
        def _():
            relayed(-1, i)
            relayed(1, i)

        @pl.when(jnp.logical_not(end))
        def _():
            pl.when(i % 2 == 0)(lambda: relayed(-1, i // 2))
            pl.when(i % 2 == 1)(lambda: relayed(1, i // 2))

    landed(c_recv.at[0], len(FIRST) * count)
    columns(FIRST, 0)

    @pl.loop(0, count)
    def _(i):
        multiply(FIRST, chunk(i), False)
        from_line(-3, i)
        from_line(3, i)
        from_cross(-2, i)
        from_cross(2, i)

        @pl.when(end)
        def _():
            relayed(-2, i)
            relayed(2, i)

        @pl.when(jnp.logical_not(end))
        def _():
            later = (count + i) // 2
            pl.when(i % 2 == 0)(lambda: relayed(-1, later))
            pl.when(i % 2 == 1)(lambda: relayed(1, later))

        @pl.when(end & (i > early))
        def _():
            relayed(-3, i - early - 1)
            relayed(3, i - early - 1)

        @pl.when(end & (i == early))
        def _():
            landed(c_recv.at[2], len(SECOND) * early)
            columns(SECOND, 1)

        @pl.when(end & (i >= early))
        def _():
            multiply(SECOND, chunk(i - early), True)

    @pl.when(jnp.logical_not(end))
    def _():
        landed(c_recv.at[2], len(SECOND) * early)
        for i in range(early, count):
            landed(c_recv.at[3 + i - early], len(SECOND))
        columns(SECOND, 1)

    ahead = count - early - 1

    @pl.loop(0, count)
    def _(i):
        @pl.when(end & (i % 2 == 0))
        def _():
            relayed(-3, ahead + i // 2)
            relayed(3, ahead + i // 2)

        @pl.when(end & ((i == 2) | (i == 4)))
        def _():
            from_cross(-3, count - 3 + i // 2)
            from_cross(3, count - 3 + i // 2)

        @pl.when(jnp.logical_not(end))
        def _():
            relayed(-2, i)
            relayed(2, i)

        later = jnp.where(end, i + count - early, i)

        @pl.when(later < count)
        def _():
            pl.when(end)(lambda: landed(c_recv.at[3 + i], len(SECOND)))
            multiply(SECOND, chunk(later), True)

    landed(c_recv.at[1], count)
    pl.when(jnp.logical_not(owns))(lambda: landed(y_recv.at[2], 2))
    landed(c_send, CHIPS * count)
    pl.when(owns)(lambda: landed(y_send, 2 * CHIPS))
    for zz in range(LINE):
        @pl.when(z == zz)
        def _():
            landed(x_send, CROSSING[zz] + sum(count - c for c in CROSSING))
            if zz < LINE - 1:
                landed(z_send.at[1], sum(count + c for c in CROSSING[:zz + 1]))
            if zz > 0:
                landed(z_send.at[0], sum(count + c for c in CROSSING[zz:]))


def gather(grad_hidden, gate, width, tokens):
    mine, hidden = gate.shape
    count = hidden // width
    sem = pltpu.SemaphoreType.DMA
    vmem = pl.BlockSpec(memory_space=pltpu.VMEM)
    held = hidden * tokens * 2 + width * tokens * 2 + hidden * width * 4
    return pl.pallas_call(
        functools.partial(gather_kernel, (count, width)),
        out_shape=(
            pltpu.VMEM((hidden, tokens), jnp.bfloat16),
            pltpu.VMEM((width, tokens), jnp.bfloat16),
            pltpu.VMEM((hidden, width), jnp.float32),
        ),
        in_specs=[pl.BlockSpec(memory_space=pl.ANY)] * 2,
        out_specs=(vmem, vmem, vmem),
        scratch_shapes=[
            pltpu.VMEM((2, mine, width), jnp.bfloat16),
            pltpu.VMEM((2, mine, width), jnp.bfloat16),
            sem((2,)),
            sem((2,)),
            sem((2,)),
            sem(()),
            sem(()),
            sem(()),
            sem((CHIPS, count)),
            sem((3 + count - count // 2,)),
            sem((3,)),
        ],
        compiler_params=pltpu.CompilerParams(
            collective_id=0, has_side_effects=True, vmem_limit_bytes=VMEM_BYTES - held - 2**18
        ),
    )(grad_hidden, gate)


def finish_kernel(total, tile, all_ref, panel_ref, _, o_ref, part_ref, b_ref, sem):
    me, t, z, x, core = position()
    width = panel_ref.shape[0]
    count = all_ref.shape[0] // width
    lanes = pl.ds(LAST * 2 * LANES, 2 * LANES)

    for ours in (True, False):
        @pl.when((me // count == t) == ours)
        def _():
            rows = pl.ds(pl.multiple_of(me % count * width, width), width)
            b_ref[...] = all_ref[rows, lanes] if ours else panel_ref[:, lanes]

    def rows_of(i):
        return pl.ds(pl.multiple_of(i * tile, tile), tile)

    def out(i):
        return pltpu.make_async_copy(part_ref.at[rows_of(i)], o_ref.at[rows_of(i)], sem.at[i])

    steps = o_ref.shape[0] // tile

    @pl.loop(0, steps)
    def _(i):
        product = nt_dot(all_ref[rows_of(i), lanes], b_ref[...])
        part_ref[rows_of(i), :] = (part_ref[rows_of(i), :] + product) * (1.0 / total)
        out(i).start()

    @pl.loop(0, steps)
    def _(i):
        out(i).wait()


def finish(everything, panel, part, tile):
    hidden, tokens = everything.shape
    width = panel.shape[0]
    held = hidden * tokens * 2 + width * tokens * 2 + hidden * width * 4
    keep = lambda array: pltpu.with_memory_space_constraint(array, pltpu.VMEM)
    vmem = pl.BlockSpec(memory_space=pltpu.VMEM)
    return pl.pallas_call(
        functools.partial(finish_kernel, tokens, tile),
        out_shape=(
            jax.ShapeDtypeStruct((hidden, width), jnp.float32),
            pltpu.VMEM((hidden, width), jnp.float32),
        ),
        in_specs=[vmem] * 3,
        out_specs=(pl.BlockSpec(memory_space=pl.ANY), vmem),
        input_output_aliases={2: 1},
        scratch_shapes=[
            pltpu.VMEM((width, 2 * LANES), jnp.bfloat16),
            pltpu.SemaphoreType.DMA((hidden // tile,)),
        ],
        compiler_params=pltpu.CompilerParams(vmem_limit_bytes=VMEM_BYTES - held - 2**18),
    )(keep(everything), keep(panel), keep(part))[0]


def shards(grad_hidden, gate):
    tensor_count, data_count = lax.axis_size("tensor"), lax.axis_size("dp")
    mine, hidden = grad_hidden.shape
    width = hidden * tensor_count // data_count
    tokens = mine * data_count
    held = hidden * tokens * 2 + width * tokens * 2 + hidden * width * 4
    fits = (
        tensor_count == 2 and data_count == 4 * LINE and mine == LANES and width % LANES == 0
        and tokens & (tokens - 1) == 0 and held + 7 * 2**20 < VMEM_BYTES
    )
    if not fits:
        return plain(grad_hidden, gate)
    everything, panel, part = gather(grad_hidden, gate, width, tokens)
    return finish(everything, panel, part, width // 2)


def solution(mesh):
    return jax.shard_map(
        shards,
        mesh=mesh,
        in_specs=(P("dp", "tensor"), P("dp", "tensor")),
        out_specs=P("tensor", "dp"),
        check_vma=False,
    )
```

```python
import functools

import jax
import jax.numpy as jnp
from jax import lax
from jax.experimental import pallas as pl
from jax.experimental.pallas import tpu as pltpu
from jax.sharding import PartitionSpec as P

MESH = pl.DeviceIdType.MESH
LANES = 128
LINE = 4
CHIPS = 2 * LINE
VMEM_BYTES = 67_043_328

BOTTOM = {
    0: [(0, 0), (0, 1), (1, 0), (2, 0), (1, 1), (3, 0), (2, 1), (3, 1)],
    1: [(1, 0), (1, 1), (0, 0), (2, 0), (3, 0), (0, 1), (2, 1), (3, 1)],
}
ORDER = [BOTTOM[z] if z in BOTTOM else [(LINE - 1 - a, r) for a, r in BOTTOM[LINE - 1 - z]] for z in range(LINE)]
FIRST, SECOND = range(0, 5), range(5, 7)
LAST = CHIPS - 1
READY = 2
CROSSING = [2 if z in (0, LINE - 1) else 1 for z in range(LINE)]


def activations(grad_hidden, gate):
    return (grad_hidden.astype(jnp.float32) * jax.nn.silu(gate.astype(jnp.float32))).astype(
        jnp.bfloat16
    )


def plain(grad_hidden, gate):
    up_grad = activations(grad_hidden, gate)
    tensor_count = lax.axis_size("tensor")
    data_count = lax.axis_size("dp")
    col_width = up_grad.shape[1] * tensor_count // data_count
    ratio = data_count // tensor_count
    data_index = lax.axis_index("dp")
    owner = data_index // ratio
    offset = data_index % ratio * col_width
    contract = (((0,), (0,)), ((), ()))
    total_tokens = up_grad.shape[0] * data_count
    rows_all = lax.all_gather(up_grad, "dp", axis=0, tiled=True)
    panel = lax.dynamic_slice_in_dim(rows_all, offset, col_width, 1)
    slices = lax.all_gather(panel, "tensor", axis=1, tiled=True)
    cols_all = lax.dynamic_slice_in_dim(slices, owner * col_width, col_width, 1)
    summed = lax.dot_general(rows_all, cols_all, contract, preferred_element_type=jnp.float32)
    return summed / total_tokens


def pick(index, values):
    known = [v for v in values if v is not None]
    if all(v == known[0] for v in known):
        return jnp.int32(known[0])
    out = jnp.int32(known[-1])
    for j, v in enumerate(values):
        if v is not None and v != known[-1]:
            out = jnp.where(index == j, v, out)
    return out


def slot_at(z, shift, d, r):
    def one(zz):
        if not (0 <= zz + d < LINE and 0 <= zz + shift < LINE):
            return None
        return ORDER[zz + shift].index((zz + d, r))
    return pick(z, [one(zz) for zz in range(LINE)])


def nt_dot(a, b):
    return lax.dot_general(a, b, (((1,), (1,)), ((), ())), preferred_element_type=jnp.float32)


def position():
    me, t = lax.axis_index("dp"), lax.axis_index("tensor")
    return me, t, me // 4, me // 2 % 2, me % 2


def gather_kernel(
    dims, g_ref, v_ref, all_ref, panel_ref, part_ref, g_buf, v_buf, g_sem, v_sem,
    z_send, x_send, c_send, y_send, recv, tail, c_recv, y_recv,
):
    count, rows, total = dims
    me, t, z, x, core = position()
    here = me // 2
    half = CHIPS // 2
    early = count // 2
    owns = here // half == t
    part = here % half
    end = (z == 0) | (z == LINE - 1)
    has_up, has_down = z < LINE - 1, z > 0

    up = (jnp.minimum(z + 1, LINE - 1) * 4 + x * 2 + core, t)
    down = (jnp.maximum(z - 1, 0) * 4 + x * 2 + core, t)
    over = (z * 4 + (1 - x) * 2 + core, t)
    twin = (z * 4 + x * 2 + 1 - core, t)

    def chunk(i):
        return jnp.where(t == 0, i, count - 1 - i)

    def rows_of(k):
        return pl.ds(pl.multiple_of(k * rows, rows), rows)

    def inputs(i):
        return [
            pltpu.make_async_copy(src.at[:, rows_of(chunk(i))], dst.at[i % 2], sem.at[i % 2])
            for src, dst, sem in ((g_ref, g_buf, g_sem), (v_ref, v_buf, v_sem))
        ]

    for copy in inputs(0):
        copy.start()

    barrier = pltpu.get_barrier_semaphore()
    greet = lambda dev: pl.semaphore_signal(barrier, inc=1, device_id=dev, device_id_type=MESH)
    greet(over)
    greet(twin)
    greet((me, 1 - t))
    greet(twin[:1] + (1 - t,))
    pl.when(has_up)(lambda: greet(up))
    pl.when(has_down)(lambda: greet(down))

    def lanes_of(slot, c):
        return pl.ds(pl.multiple_of((slot * 2 + c) * LANES, LANES), LANES)

    def number(d, r):
        return (z + d) * 2 + (1 - x if r else x)

    def place(shift, d, r, i, h=None):
        k, lanes = chunk(i), lanes_of(slot_at(z, shift, d, r), core)
        if h is None:
            return all_ref.at[rows_of(k), lanes]
        return all_ref.at[pl.ds(pl.multiple_of(k * rows + h * (rows // 2), rows // 2), rows // 2), lanes]

    def along(d, r, i, way, h=None):
        return pltpu.make_async_remote_copy(
            src_ref=place(0, d, r, i, h), dst_ref=place(1 if way else -1, d, r, i, h),
            send_sem=z_send.at[way], recv_sem=tail.at[1] if h else recv.at[number(d, r), i],
            device_id=(down, up)[way], device_id_type=MESH)

    def across(d, r, i, h=None):
        return pltpu.make_async_remote_copy(
            src_ref=place(0, d, r, i, h), dst_ref=place(0, d, 1 - r, i, h),
            send_sem=x_send, recv_sem=tail.at[0] if h else recv.at[number(d, r), i],
            device_id=over, device_id_type=MESH)

    def to_twin(d, r, i, h=None):
        slot = slot_at(z, 0, d, r)
        later = 2 + jnp.maximum(i - early + 1, 0)
        final = jnp.where(i < early, 1, 3 + count - early)
        index = jnp.where(slot < SECOND[0], 0, jnp.where(slot == LAST, final, later))
        return pltpu.make_async_remote_copy(
            src_ref=place(0, d, r, i, h), dst_ref=place(0, d, r, i, h), send_sem=c_send,
            recv_sem=c_recv.at[index], device_id=twin, device_id_type=MESH)

    def to_panel(d, r, i):
        k, slot = chunk(i), slot_at(z, 0, d, r)
        index = jnp.where(slot < SECOND[0], 0, jnp.where(slot == LAST, 2, 1))
        return pltpu.make_async_remote_copy(
            src_ref=place(0, d, r, i), dst_ref=panel_ref.at[:, lanes_of(slot, core)],
            send_sem=y_send, recv_sem=y_recv.at[index],
            device_id=(here * 2 + k % 2, 1 - t), device_id_type=MESH)

    def spread_panel(d, r, i):
        pl.when(owns & (chunk(i) // 2 == part))(lambda: to_panel(d, r, i).start())

    def spread(d, r, i):
        to_twin(d, r, i).start()
        spread_panel(d, r, i)

    def take_halves(d, i, mark):
        for h, sem in enumerate((recv.at[number(d, 1), i], tail.at[mark])):
            piece = all_ref.at[pl.ds(0, rows // 8), pl.ds(0, 4 * LANES)]
            pltpu.make_async_copy(piece, piece, sem).wait()
            to_twin(d, 1, i, h).start()
        spread_panel(d, 1, i)

    def landed(sem, chunks=1):
        piece = all_ref.at[pl.ds(0, chunks * rows // 8), pl.ds(0, 8 * LANES)]
        pltpu.make_async_copy(piece, piece, sem).wait()

    def arrive(d, r, i):
        landed(recv.at[number(d, r), i])

    def straight(d):
        return pick(z, [count - CROSSING[zz + d] if 0 <= zz + d < LINE else None for zz in range(LINE)])

    def exists(d):
        return (z + d >= 0) & (z + d < LINE)

    def both_ways(d, r, i):
        pl.when(has_up)(lambda: along(d, r, i, 1).start())
        pl.when(has_down)(lambda: along(d, r, i, 0).start())

    def onward(d, r, i):
        if abs(d) == LINE - 1:
            return
        way = 1 if d < 0 else 0
        goes = has_up if way else has_down
        if abs(d) < LINE - 2 or r == 0:
            pl.when(goes)(lambda: along(d, r, i, way).start())
            return
        pl.when(goes & (i < count - 1))(lambda: along(d, r, i, way).start())

        @pl.when(goes & (i == count - 1))
        def _():
            along(d, r, i, way, 0).start()
            along(d, r, i, way, 1).start()

    def flip(i):
        for copy in inputs(i):
            copy.wait()
        columns = rows_of(chunk(i))
        v = v_buf[i % 2].astype(jnp.float32)
        u = g_buf[i % 2].astype(jnp.float32) * (v / (1.0 + jnp.exp(-v)))
        all_ref[columns, lanes_of(0, core)] = u.astype(jnp.bfloat16).T

    def send_own(i):
        both_ways(0, 0, i)
        across(0, 0, i).start()
        spread(0, 0, i)

    def fetch(i):
        for copy in inputs(i):
            copy.start()

    flip(0)
    fetch(1)
    pl.semaphore_wait(barrier, jnp.where(end, 5, 6))
    send_own(0)
    fetch(2)
    flip(1)

    @pl.loop(2, count)
    def _(i):
        pl.when(i + 1 < count)(lambda: fetch(i + 1))
        flip(i)
        send_own(i - 1)

    send_own(count - 1)

    def from_line(d, i):
        @pl.when(exists(d))
        def _():
            arrive(d, 0, i)
            onward(d, 0, i)
            whole = straight(d) - (1 if abs(d) == LINE - 1 else 0)
            pl.when(i < whole)(lambda: across(d, 0, i).start())
            if abs(d) == LINE - 1:
                @pl.when(i == whole)
                def _():
                    across(d, 0, i, 0).start()
                    across(d, 0, i, 1).start()
            spread(d, 0, i)

    def from_cross(d, i):
        @pl.when(exists(d) & (i >= straight(d)))
        def _():
            def take():
                arrive(d, 1, i)
                onward(d, 1, i)
                spread(d, 1, i)

            if abs(d) < LINE - 1:
                take()
            else:
                pl.when(i < count - 1)(take)
                pl.when(i == count - 1)(lambda: take_halves(d, i, 1))

    def relayed(d, i):
        @pl.when(exists(d) & (i < straight(d)))
        def _():
            def take():
                arrive(d, 1, i)
                spread(d, 1, i)

            if abs(d) < LINE - 1:
                take()
            else:
                pl.when(i < straight(d) - 1)(take)
                pl.when(i == straight(d) - 1)(lambda: take_halves(d, i, 0))

    def neighbour(i):
        arrive(0, 1, i)
        pl.when(i >= straight(0))(lambda: both_ways(0, 1, i))
        spread(0, 1, i)

    def span(slots):
        return pl.ds(slots[0] * 2 * LANES, len(slots) * 2 * LANES)

    def columns(slots, group):
        pl.when(jnp.logical_not(owns))(lambda: landed(y_recv.at[group], 2 * len(slots)))

        @pl.when(owns)
        def _():
            panel_ref[:, span(slots)] = all_ref[rows_of(me % count), span(slots)]

    def multiply(slots, k, add, scale=None):
        product = nt_dot(all_ref[rows_of(k), span(slots)], panel_ref[:, span(slots)])
        if add:
            product += part_ref[rows_of(k), :]
        part_ref[rows_of(k), :] = product if scale is None else product * scale

    @pl.loop(0, count)
    def _(i):
        from_line(-1, i)
        from_line(1, i)
        neighbour(i)

    @pl.loop(0, count)
    def _(i):
        from_line(-2, i)
        from_line(2, i)
        from_cross(-1, i)
        from_cross(1, i)

        @pl.when(end)
        def _():
            relayed(-1, i)
            relayed(1, i)

        @pl.when(jnp.logical_not(end))
        def _():
            pl.when(i % 2 == 0)(lambda: relayed(-1, i // 2))
            pl.when(i % 2 == 1)(lambda: relayed(1, i // 2))

    landed(c_recv.at[0], len(FIRST) * count)
    columns(FIRST, 0)

    @pl.loop(0, count)
    def _(i):
        multiply(FIRST, chunk(i), False)
        from_line(-3, i)
        from_line(3, i)

        @pl.when(end)
        def _():
            relayed(-2, i)
            relayed(2, i)

        @pl.when(jnp.logical_not(end))
        def _():
            from_cross(-2, i)
            from_cross(2, i)
            later = (count + i) // 2
            pl.when(i % 2 == 0)(lambda: relayed(-1, later))
            pl.when(i % 2 == 1)(lambda: relayed(1, later))

        @pl.when(end & (i > early))
        def _():
            relayed(-3, i - early - 1)
            relayed(3, i - early - 1)

        @pl.when(end & (i == early))
        def _():
            landed(c_recv.at[2], len(SECOND) * early)
            columns(SECOND, 1)

        @pl.when(end & (i >= early))
        def _():
            multiply(SECOND, chunk(i - early), True)

    @pl.when(jnp.logical_not(end))
    def _():
        landed(c_recv.at[2], len(SECOND) * early)
        for i in range(early, count):
            landed(c_recv.at[3 + i - early], len(SECOND))
        columns(SECOND, 1)

    ahead = count - early - 1

    @pl.loop(0, count)
    def _(i):
        @pl.when(end & (i % 2 == 0))
        def _():
            relayed(-3, ahead + i // 2)
            relayed(3, ahead + i // 2)

        @pl.when(end & (i == 0))
        def _():
            from_cross(-2, count - 1)
            from_cross(2, count - 1)

        @pl.when(end & ((i == 2) | (i == 4)))
        def _():
            from_cross(-3, count - 3 + i // 2)
            from_cross(3, count - 3 + i // 2)

        @pl.when(jnp.logical_not(end))
        def _():
            relayed(-2, i)
            relayed(2, i)

        later = jnp.where(end, i + count - early, i)

        @pl.when(later < count)
        def _():
            pl.when(end)(lambda: landed(c_recv.at[3 + i], len(SECOND)))
            multiply(SECOND, chunk(later), True)

        @pl.when(i == jnp.where(end, early - 1, count - 1))
        def _():
            landed(c_recv.at[1], early)
            pl.when(jnp.logical_not(end))(lambda: landed(c_recv.at[3 + count - early], count - early))
            columns([LAST], 2)

            @pl.loop(0, READY)
            def _(j):
                multiply([LAST], chunk(j), True, 1.0 / total)

    pl.when(end)(lambda: landed(c_recv.at[3 + count - early], count - early))
    landed(c_send, CHIPS * count)
    pl.when(owns)(lambda: landed(y_send, 2 * CHIPS))
    for zz in range(LINE):
        @pl.when(z == zz)
        def _():
            landed(x_send, CROSSING[zz] + sum(count - c for c in CROSSING))
            if zz < LINE - 1:
                landed(z_send.at[1], sum(count + c for c in CROSSING[:zz + 1]))
            if zz > 0:
                landed(z_send.at[0], sum(count + c for c in CROSSING[zz:]))


def gather(grad_hidden, gate, width, tokens):
    mine, hidden = gate.shape
    count = hidden // width
    sem = pltpu.SemaphoreType.DMA
    vmem = pl.BlockSpec(memory_space=pltpu.VMEM)
    held = hidden * tokens * 2 + width * tokens * 2 + hidden * width * 4
    return pl.pallas_call(
        functools.partial(gather_kernel, (count, width, tokens)),
        out_shape=(
            pltpu.VMEM((hidden, tokens), jnp.bfloat16),
            pltpu.VMEM((width, tokens), jnp.bfloat16),
            pltpu.VMEM((hidden, width), jnp.float32),
        ),
        in_specs=[pl.BlockSpec(memory_space=pl.ANY)] * 2,
        out_specs=(vmem, vmem, vmem),
        scratch_shapes=[
            pltpu.VMEM((2, mine, width), jnp.bfloat16),
            pltpu.VMEM((2, mine, width), jnp.bfloat16),
            sem((2,)),
            sem((2,)),
            sem((2,)),
            sem(()),
            sem(()),
            sem(()),
            sem((CHIPS, count)),
            sem((2,)),
            sem((4 + count - count // 2,)),
            sem((3,)),
        ],
        compiler_params=pltpu.CompilerParams(
            collective_id=0, has_side_effects=True, vmem_limit_bytes=VMEM_BYTES - held - 2**18
        ),
    )(grad_hidden, gate)


def finish_kernel(total, split, all_ref, panel_ref, _, o_ref, part_ref, sem):
    t, width = lax.axis_index("tensor"), panel_ref.shape[0]
    count, tile = all_ref.shape[0] // width, width // split
    lanes = pl.ds(LAST * 2 * LANES, 2 * LANES)

    def rows_of(j):
        k = jnp.where(t == 0, j // split, count - 1 - j // split)
        return pl.ds(pl.multiple_of(k * width + j % split * tile, tile), tile)

    def out(j):
        return pltpu.make_async_copy(part_ref.at[rows_of(j)], o_ref.at[rows_of(j)], sem.at[j])

    @pl.loop(0, READY * split)
    def _(j):
        out(j).start()

    @pl.loop(READY * split, count * split)
    def _(j):
        product = nt_dot(all_ref[rows_of(j), lanes], panel_ref[:, lanes])
        part_ref[rows_of(j), :] = (part_ref[rows_of(j), :] + product) * (1.0 / total)
        out(j).start()

    @pl.loop(0, count * split)
    def _(j):
        out(j).wait()


def finish(everything, panel, part, split):
    hidden, tokens = everything.shape
    width = panel.shape[0]
    held = hidden * tokens * 2 + width * tokens * 2 + hidden * width * 4
    keep = lambda array: pltpu.with_memory_space_constraint(array, pltpu.VMEM)
    vmem = pl.BlockSpec(memory_space=pltpu.VMEM)
    return pl.pallas_call(
        functools.partial(finish_kernel, tokens, split),
        out_shape=(
            jax.ShapeDtypeStruct((hidden, width), jnp.float32),
            pltpu.VMEM((hidden, width), jnp.float32),
        ),
        in_specs=[vmem] * 3,
        out_specs=(pl.BlockSpec(memory_space=pl.ANY), vmem),
        input_output_aliases={2: 1},
        scratch_shapes=[
            pltpu.SemaphoreType.DMA((hidden // width * split,)),
        ],
        compiler_params=pltpu.CompilerParams(vmem_limit_bytes=VMEM_BYTES - held - 2**18),
    )(keep(everything), keep(panel), keep(part))[0]


def shards(grad_hidden, gate):
    tensor_count, data_count = lax.axis_size("tensor"), lax.axis_size("dp")
    mine, hidden = grad_hidden.shape
    width = hidden * tensor_count // data_count
    tokens = mine * data_count
    held = hidden * tokens * 2 + width * tokens * 2 + hidden * width * 4
    fits = (
        tensor_count == 2 and data_count == 4 * LINE and mine == LANES and width % LANES == 0
        and tokens & (tokens - 1) == 0 and held + 7 * 2**20 < VMEM_BYTES
    )
    if not fits:
        return plain(grad_hidden, gate)
    everything, panel, part = gather(grad_hidden, gate, width, tokens)
    return finish(everything, panel, part, 2)


def solution(mesh):
    return jax.shard_map(
        shards,
        mesh=mesh,
        in_specs=(P("dp", "tensor"), P("dp", "tensor")),
        out_specs=P("tensor", "dp"),
        check_vma=False,
    )
```

```python
import functools

import jax
import jax.numpy as jnp
from jax import lax
from jax.experimental import pallas as pl
from jax.experimental.pallas import tpu as pltpu
from jax.sharding import PartitionSpec as P

MESH = pl.DeviceIdType.MESH
LANES = 128
LINE = 4
CHIPS = 2 * LINE
VMEM_BYTES = 67_043_328

BOTTOM = {
    0: [(0, 0), (0, 1), (1, 0), (2, 0), (1, 1), (3, 0), (2, 1), (3, 1)],
    1: [(1, 0), (1, 1), (0, 0), (2, 0), (3, 0), (0, 1), (2, 1), (3, 1)],
}
ORDER = [BOTTOM[z] if z in BOTTOM else [(LINE - 1 - a, r) for a, r in BOTTOM[LINE - 1 - z]] for z in range(LINE)]
FIRST, SECOND = range(0, 5), range(5, 7)
LAST = CHIPS - 1
READY = 2
CROSSING = [2 if z in (0, LINE - 1) else 1 for z in range(LINE)]


def activations(grad_hidden, gate):
    return (grad_hidden.astype(jnp.float32) * jax.nn.silu(gate.astype(jnp.float32))).astype(
        jnp.bfloat16
    )


def plain(grad_hidden, gate):
    up_grad = activations(grad_hidden, gate)
    tensor_count = lax.axis_size("tensor")
    data_count = lax.axis_size("dp")
    col_width = up_grad.shape[1] * tensor_count // data_count
    ratio = data_count // tensor_count
    data_index = lax.axis_index("dp")
    owner = data_index // ratio
    offset = data_index % ratio * col_width
    contract = (((0,), (0,)), ((), ()))
    total_tokens = up_grad.shape[0] * data_count
    rows_all = lax.all_gather(up_grad, "dp", axis=0, tiled=True)
    panel = lax.dynamic_slice_in_dim(rows_all, offset, col_width, 1)
    slices = lax.all_gather(panel, "tensor", axis=1, tiled=True)
    cols_all = lax.dynamic_slice_in_dim(slices, owner * col_width, col_width, 1)
    summed = lax.dot_general(rows_all, cols_all, contract, preferred_element_type=jnp.float32)
    return summed / total_tokens


def pick(index, values):
    known = [v for v in values if v is not None]
    if all(v == known[0] for v in known):
        return jnp.int32(known[0])
    out = jnp.int32(known[-1])
    for j, v in enumerate(values):
        if v is not None and v != known[-1]:
            out = jnp.where(index == j, v, out)
    return out


def slot_at(z, shift, d, r):
    def one(zz):
        if not (0 <= zz + d < LINE and 0 <= zz + shift < LINE):
            return None
        return ORDER[zz + shift].index((zz + d, r))
    return pick(z, [one(zz) for zz in range(LINE)])


def nt_dot(a, b):
    return lax.dot_general(a, b, (((1,), (1,)), ((), ())), preferred_element_type=jnp.float32)


def position():
    me, t = lax.axis_index("dp"), lax.axis_index("tensor")
    return me, t, me // 4, me // 2 % 2, me % 2


def gather_kernel(
    dims, g_ref, v_ref, all_ref, panel_ref, part_ref, g_buf, v_buf, g_sem, v_sem,
    z_send, x_send, c_send, y_send, recv, tail, c_recv, y_recv,
):
    count, rows, total = dims
    me, t, z, x, core = position()
    here = me // 2
    half = CHIPS // 2
    early = count // 2
    owns = here // half == t
    part = here % half
    end = (z == 0) | (z == LINE - 1)
    has_up, has_down = z < LINE - 1, z > 0

    up = (jnp.minimum(z + 1, LINE - 1) * 4 + x * 2 + core, t)
    down = (jnp.maximum(z - 1, 0) * 4 + x * 2 + core, t)
    over = (z * 4 + (1 - x) * 2 + core, t)
    twin = (z * 4 + x * 2 + 1 - core, t)

    def chunk(i):
        return jnp.where(t == 0, i, count - 1 - i)

    def rows_of(k):
        return pl.ds(pl.multiple_of(k * rows, rows), rows)

    def inputs(i):
        return [
            pltpu.make_async_copy(src.at[:, rows_of(chunk(i))], dst.at[i % 2], sem.at[i % 2])
            for src, dst, sem in ((g_ref, g_buf, g_sem), (v_ref, v_buf, v_sem))
        ]

    barrier = pltpu.get_barrier_semaphore()
    greet = lambda dev: pl.semaphore_signal(barrier, inc=1, device_id=dev, device_id_type=MESH)
    pl.when(has_up)(lambda: greet(up))
    pl.when(has_down)(lambda: greet(down))
    greet(over)
    for copy in inputs(0):
        copy.start()
    greet(twin)
    greet((me, 1 - t))
    greet(twin[:1] + (1 - t,))

    def lanes_of(slot, c):
        return pl.ds(pl.multiple_of((slot * 2 + c) * LANES, LANES), LANES)

    def number(d, r):
        return (z + d) * 2 + (1 - x if r else x)

    def place(shift, d, r, i, h=None):
        k, lanes = chunk(i), lanes_of(slot_at(z, shift, d, r), core)
        if h is None:
            return all_ref.at[rows_of(k), lanes]
        return all_ref.at[pl.ds(pl.multiple_of(k * rows + h * (rows // 2), rows // 2), rows // 2), lanes]

    def along(d, r, i, way, h=None):
        return pltpu.make_async_remote_copy(
            src_ref=place(0, d, r, i, h), dst_ref=place(1 if way else -1, d, r, i, h),
            send_sem=z_send.at[way], recv_sem=tail.at[1] if h else recv.at[number(d, r), i],
            device_id=(down, up)[way], device_id_type=MESH)

    def across(d, r, i, h=None):
        return pltpu.make_async_remote_copy(
            src_ref=place(0, d, r, i, h), dst_ref=place(0, d, 1 - r, i, h),
            send_sem=x_send, recv_sem=tail.at[0] if h else recv.at[number(d, r), i],
            device_id=over, device_id_type=MESH)

    def to_twin(d, r, i, h=None):
        slot = slot_at(z, 0, d, r)
        later = 2 + jnp.maximum(i - early + 1, 0)
        final = jnp.where(i < early, 1, 3 + count - early)
        index = jnp.where(slot < SECOND[0], 0, jnp.where(slot == LAST, final, later))
        return pltpu.make_async_remote_copy(
            src_ref=place(0, d, r, i, h), dst_ref=place(0, d, r, i, h), send_sem=c_send,
            recv_sem=c_recv.at[index], device_id=twin, device_id_type=MESH)

    def to_panel(d, r, i):
        k, slot = chunk(i), slot_at(z, 0, d, r)
        index = jnp.where(slot < SECOND[0], 0, jnp.where(slot == LAST, 2, 1))
        return pltpu.make_async_remote_copy(
            src_ref=place(0, d, r, i), dst_ref=panel_ref.at[:, lanes_of(slot, core)],
            send_sem=y_send, recv_sem=y_recv.at[index],
            device_id=(here * 2 + k % 2, 1 - t), device_id_type=MESH)

    def spread_panel(d, r, i):
        pl.when(owns & (chunk(i) // 2 == part))(lambda: to_panel(d, r, i).start())

    def spread(d, r, i):
        to_twin(d, r, i).start()
        spread_panel(d, r, i)

    def take_halves(d, i, mark):
        for h, sem in enumerate((recv.at[number(d, 1), i], tail.at[mark])):
            piece = all_ref.at[pl.ds(0, rows // 8), pl.ds(0, 4 * LANES)]
            pltpu.make_async_copy(piece, piece, sem).wait()
            to_twin(d, 1, i, h).start()
        spread_panel(d, 1, i)

    def landed(sem, chunks=1):
        piece = all_ref.at[pl.ds(0, chunks * rows // 8), pl.ds(0, 8 * LANES)]
        pltpu.make_async_copy(piece, piece, sem).wait()

    def arrive(d, r, i):
        landed(recv.at[number(d, r), i])

    def straight(d):
        return pick(z, [count - CROSSING[zz + d] if 0 <= zz + d < LINE else None for zz in range(LINE)])

    def exists(d):
        return (z + d >= 0) & (z + d < LINE)

    def both_ways(d, r, i):
        pl.when(has_up)(lambda: along(d, r, i, 1).start())
        pl.when(has_down)(lambda: along(d, r, i, 0).start())

    def onward(d, r, i):
        if abs(d) == LINE - 1:
            return
        way = 1 if d < 0 else 0
        goes = has_up if way else has_down
        if abs(d) < LINE - 2 or r == 0:
            pl.when(goes)(lambda: along(d, r, i, way).start())
            return
        pl.when(goes & (i < count - 1))(lambda: along(d, r, i, way).start())

        @pl.when(goes & (i == count - 1))
        def _():
            along(d, r, i, way, 0).start()
            along(d, r, i, way, 1).start()

    def flip(i):
        for copy in inputs(i):
            copy.wait()
        columns = rows_of(chunk(i))
        v = v_buf[i % 2].astype(jnp.float32)
        u = g_buf[i % 2].astype(jnp.float32) * (v / (1.0 + jnp.exp(-v)))
        all_ref[columns, lanes_of(0, core)] = u.astype(jnp.bfloat16).T

    def send_own(i):
        both_ways(0, 0, i)
        across(0, 0, i).start()
        spread(0, 0, i)

    def fetch(i):
        for copy in inputs(i):
            copy.start()

    flip(0)
    fetch(1)
    pl.semaphore_wait(barrier, jnp.where(end, 5, 6))
    send_own(0)
    fetch(2)
    flip(1)

    @pl.loop(2, count)
    def _(i):
        pl.when(i + 1 < count)(lambda: fetch(i + 1))
        flip(i)
        send_own(i - 1)

    send_own(count - 1)

    def from_line(d, i):
        @pl.when(exists(d))
        def _():
            arrive(d, 0, i)
            onward(d, 0, i)
            whole = straight(d) - (1 if abs(d) == LINE - 1 else 0)
            pl.when(i < whole)(lambda: across(d, 0, i).start())
            if abs(d) == LINE - 1:
                @pl.when(i == whole)
                def _():
                    across(d, 0, i, 0).start()
                    across(d, 0, i, 1).start()
            spread(d, 0, i)

    def from_cross(d, i):
        @pl.when(exists(d) & (i >= straight(d)))
        def _():
            def take():
                arrive(d, 1, i)
                onward(d, 1, i)
                spread(d, 1, i)

            if abs(d) < LINE - 1:
                take()
            else:
                pl.when(i < count - 1)(take)
                pl.when(i == count - 1)(lambda: take_halves(d, i, 1))

    def relayed(d, i):
        @pl.when(exists(d) & (i < straight(d)))
        def _():
            def take():
                arrive(d, 1, i)
                spread(d, 1, i)

            if abs(d) < LINE - 1:
                take()
            else:
                pl.when(i < straight(d) - 1)(take)
                pl.when(i == straight(d) - 1)(lambda: take_halves(d, i, 0))

    def neighbour(i):
        arrive(0, 1, i)
        pl.when(i >= straight(0))(lambda: both_ways(0, 1, i))
        spread(0, 1, i)

    def span(slots):
        return pl.ds(slots[0] * 2 * LANES, len(slots) * 2 * LANES)

    def columns(slots, group):
        pl.when(jnp.logical_not(owns))(lambda: landed(y_recv.at[group], 2 * len(slots)))

        @pl.when(owns)
        def _():
            panel_ref[:, span(slots)] = all_ref[rows_of(me % count), span(slots)]

    def multiply(slots, k, add, scale=None):
        product = nt_dot(all_ref[rows_of(k), span(slots)], panel_ref[:, span(slots)])
        if add:
            product += part_ref[rows_of(k), :]
        part_ref[rows_of(k), :] = product if scale is None else product * scale

    @pl.loop(0, count)
    def _(i):
        from_line(-1, i)
        from_line(1, i)
        neighbour(i)

    @pl.loop(0, count)
    def _(i):
        from_line(-2, i)
        from_line(2, i)
        from_cross(-1, i)
        from_cross(1, i)

        @pl.when(end)
        def _():
            relayed(-1, i)
            relayed(1, i)

        @pl.when(jnp.logical_not(end))
        def _():
            pl.when(i % 2 == 0)(lambda: relayed(-1, i // 2))
            pl.when(i % 2 == 1)(lambda: relayed(1, i // 2))

    landed(c_recv.at[0], len(FIRST) * count)
    columns(FIRST, 0)

    @pl.loop(0, count)
    def _(i):
        multiply(FIRST, chunk(i), False)
        from_line(-3, i)
        from_line(3, i)

        @pl.when(end)
        def _():
            relayed(-2, i)
            relayed(2, i)

        @pl.when(jnp.logical_not(end))
        def _():
            from_cross(-2, i)
            from_cross(2, i)
            later = (count + i) // 2
            pl.when(i % 2 == 0)(lambda: relayed(-1, later))
            pl.when(i % 2 == 1)(lambda: relayed(1, later))

        @pl.when(end & (i > early))
        def _():
            relayed(-3, i - early - 1)
            relayed(3, i - early - 1)

        @pl.when(end & (i == early))
        def _():
            landed(c_recv.at[2], len(SECOND) * early)
            columns(SECOND, 1)

        @pl.when(end & (i >= early))
        def _():
            multiply(SECOND, chunk(i - early), True)

    @pl.when(jnp.logical_not(end))
    def _():
        landed(c_recv.at[2], len(SECOND) * early)
        for i in range(early, count):
            landed(c_recv.at[3 + i - early], len(SECOND))
        columns(SECOND, 1)

    ahead = count - early - 1

    @pl.loop(0, count)
    def _(i):
        @pl.when(end & (i % 2 == 0))
        def _():
            relayed(-3, ahead + i // 2)
            relayed(3, ahead + i // 2)

        @pl.when(end & (i == 0))
        def _():
            from_cross(-2, count - 1)
            from_cross(2, count - 1)

        @pl.when(end & ((i == 2) | (i == 4)))
        def _():
            from_cross(-3, count - 3 + i // 2)
            from_cross(3, count - 3 + i // 2)

        @pl.when(jnp.logical_not(end))
        def _():
            relayed(-2, i)
            relayed(2, i)

        later = jnp.where(end, i + count - early, i)

        @pl.when(later < count)
        def _():
            pl.when(end)(lambda: landed(c_recv.at[3 + i], len(SECOND)))
            multiply(SECOND, chunk(later), True)

        @pl.when(i == jnp.where(end, early - 1, count - 1))
        def _():
            landed(c_recv.at[1], early)
            pl.when(jnp.logical_not(end))(lambda: landed(c_recv.at[3 + count - early], count - early))
            columns([LAST], 2)

            @pl.loop(0, READY)
            def _(j):
                multiply([LAST], chunk(j), True, 1.0 / total)

    pl.when(end)(lambda: landed(c_recv.at[3 + count - early], count - early))
    landed(c_send, CHIPS * count)
    pl.when(owns)(lambda: landed(y_send, 2 * CHIPS))
    for zz in range(LINE):
        @pl.when(z == zz)
        def _():
            landed(x_send, CROSSING[zz] + sum(count - c for c in CROSSING))
            if zz < LINE - 1:
                landed(z_send.at[1], sum(count + c for c in CROSSING[:zz + 1]))
            if zz > 0:
                landed(z_send.at[0], sum(count + c for c in CROSSING[zz:]))


def gather(grad_hidden, gate, width, tokens):
    mine, hidden = gate.shape
    count = hidden // width
    sem = pltpu.SemaphoreType.DMA
    vmem = pl.BlockSpec(memory_space=pltpu.VMEM)
    held = hidden * tokens * 2 + width * tokens * 2 + hidden * width * 4
    return pl.pallas_call(
        functools.partial(gather_kernel, (count, width, tokens)),
        out_shape=(
            pltpu.VMEM((hidden, tokens), jnp.bfloat16),
            pltpu.VMEM((width, tokens), jnp.bfloat16),
            pltpu.VMEM((hidden, width), jnp.float32),
        ),
        in_specs=[pl.BlockSpec(memory_space=pl.ANY)] * 2,
        out_specs=(vmem, vmem, vmem),
        scratch_shapes=[
            pltpu.VMEM((2, mine, width), jnp.bfloat16),
            pltpu.VMEM((2, mine, width), jnp.bfloat16),
            sem((2,)),
            sem((2,)),
            sem((2,)),
            sem(()),
            sem(()),
            sem(()),
            sem((CHIPS, count)),
            sem((2,)),
            sem((4 + count - count // 2,)),
            sem((3,)),
        ],
        compiler_params=pltpu.CompilerParams(
            collective_id=0, has_side_effects=True, vmem_limit_bytes=VMEM_BYTES - held - 2**18
        ),
    )(grad_hidden, gate)


def finish_kernel(total, split, all_ref, panel_ref, _, o_ref, part_ref, sem):
    t, width = lax.axis_index("tensor"), panel_ref.shape[0]
    count, tile = all_ref.shape[0] // width, width // split
    lanes = pl.ds(LAST * 2 * LANES, 2 * LANES)

    def rows_of(j):
        k = jnp.where(t == 0, j // split, count - 1 - j // split)
        return pl.ds(pl.multiple_of(k * width + j % split * tile, tile), tile)

    def out(j):
        return pltpu.make_async_copy(part_ref.at[rows_of(j)], o_ref.at[rows_of(j)], sem)

    @pl.loop(0, READY * split)
    def _(j):
        out(j).start()

    @pl.loop(READY * split, count * split)
    def _(j):
        product = nt_dot(all_ref[rows_of(j), lanes], panel_ref[:, lanes])
        part_ref[rows_of(j), :] = (part_ref[rows_of(j), :] + product) * (1.0 / total)
        out(j).start()

    pltpu.make_async_copy(part_ref, o_ref, sem).wait()


def finish(everything, panel, part, split):
    hidden, tokens = everything.shape
    width = panel.shape[0]
    held = hidden * tokens * 2 + width * tokens * 2 + hidden * width * 4
    keep = lambda array: pltpu.with_memory_space_constraint(array, pltpu.VMEM)
    vmem = pl.BlockSpec(memory_space=pltpu.VMEM)
    return pl.pallas_call(
        functools.partial(finish_kernel, tokens, split),
        out_shape=(
            jax.ShapeDtypeStruct((hidden, width), jnp.float32),
            pltpu.VMEM((hidden, width), jnp.float32),
        ),
        in_specs=[vmem] * 3,
        out_specs=(pl.BlockSpec(memory_space=pl.ANY), vmem),
        input_output_aliases={2: 1},
        scratch_shapes=[
            pltpu.SemaphoreType.DMA(()),
        ],
        compiler_params=pltpu.CompilerParams(vmem_limit_bytes=VMEM_BYTES - held - 2**18),
    )(keep(everything), keep(panel), keep(part))[0]


def shards(grad_hidden, gate):
    tensor_count, data_count = lax.axis_size("tensor"), lax.axis_size("dp")
    mine, hidden = grad_hidden.shape
    width = hidden * tensor_count // data_count
    tokens = mine * data_count
    held = hidden * tokens * 2 + width * tokens * 2 + hidden * width * 4
    fits = (
        tensor_count == 2 and data_count == 4 * LINE and mine == LANES and width % LANES == 0
        and tokens & (tokens - 1) == 0 and held + 7 * 2**20 < VMEM_BYTES
    )
    if not fits:
        return plain(grad_hidden, gate)
    everything, panel, part = gather(grad_hidden, gate, width, tokens)
    return finish(everything, panel, part, 2)


def solution(mesh):
    return jax.shard_map(
        shards,
        mesh=mesh,
        in_specs=(P("dp", "tensor"), P("dp", "tensor")),
        out_specs=P("tensor", "dp"),
        check_vma=False,
    )
```
